32 devices in a mesh: group: 2 (over core), row: 2 (over x), col: 8 (over z, y).
Axes of the slice: x: 2, y: 2, z: 4, core: 2. Of those that a mesh axis runs over, the one named last changes fastest.
Arguments:
- velocity_hat: float32 [3, 2, 4, 512, 512], P(None, None, ('group', 'row'), 'col'), may hold values from -6 to 6
- scalar: float32 [4, 1024, 1024], P('group', 'col', 'row'), may hold values from -6 to 6
- tile_offset: int32 [1], replicated, may hold values from 0 to 511
Outputs:
- velocity_new: float32 [3, 2, 4, 512, 512], P(None, None, ('group', 'row'), 'col')
- scalar_new: float32 [4, 1024, 1024], P('group', 'col', 'row')
The draws below stay inside these ranges and needn't reach their ends.
Inputs may be any that keep to these rules, and one draw needn't show every extreme that they name: `tile_offset`: one offset for every tile and plane.
All inputs are finite; a program needn't handle non-finite values.
Results may differ from the reference program's by a relative error of at most 0.000076.
Values sent between devices are 32-bit elements; how exact they have to be, the bound alone decides.
No kernel may reach another device: no remote copies, remote signals or barrier semaphores. Data moves between devices by JAX's collectives and lax.ppermute only.
A program may use at most 64 MiB of HBM per device.

```python
import jax
import jax.numpy as jnp
from jax import lax

GRID = 512
PLANES = 4
FINE = 1024


def shard_levels(key, shape, pieces, least, high):
    factor_of, own = 1.0, jax.random.fold_in(key, 6)
    for axis_at, blocks in pieces:
        steps = jnp.exp(jax.random.uniform(jax.random.fold_in(own, axis_at), (blocks,), jnp.float32, least / len(pieces), high / len(pieces)))
        factor_of = factor_of * jnp.repeat(steps, shape[axis_at] // blocks).reshape([-1 if axis == axis_at else 1 for axis in range(len(shape))])
    return factor_of


def centred(own_key, shape, scale, reach, pieces=(), kind=jnp.bfloat16):
    loudness = shard_levels(own_key, shape, pieces, -0.22, 0.18) if pieces else 1.0
    array = jax.random.normal(own_key, shape, jnp.float32) * scale * loudness
    return jnp.minimum(jnp.maximum(array, -reach), reach).astype(kind)


def setup_inputs(seed: int = 0) -> dict:
    key_of = jax.random.split(jax.random.key(seed), 4)
    velocity_hat = centred(key_of[0], (3, 2, PLANES, GRID, GRID), 1.0, 6.0, ((2, 4), (3, 8)), jnp.float32)
    scalar = centred(key_of[1], (PLANES, FINE, FINE), 1.0, 6.0, ((0, 2), (1, 8), (2, 2)), jnp.float32)
    tile_offset = jax.random.randint(key_of[2], (1,), 0, GRID).astype(jnp.int32)
    return dict(velocity_hat=velocity_hat, scalar=scalar, tile_offset=tile_offset)


time_step = 0.25
viscosity = 2.0
diffusivity = 0.15
substep = 0.2


def signed(length):
    indices = jnp.arange(length, dtype=jnp.int32)
    return jnp.where(indices < length // 2, indices, indices - length)


def plane_step(plane):
    extent = plane.shape[-1]
    wavenumber = signed(extent)
    scaled = wavenumber.astype(jnp.float32) / (extent // 2)
    kappa_x = scaled[:, None]
    kappa_y = scaled[None, :]
    spectra = plane[:, 0] + 1j * plane[:, 1]
    spin_x = 1j * kappa_y * spectra[2]
    spin_y = -1j * kappa_x * spectra[2]
    spin_z = 1j * kappa_x * spectra[1] - 1j * kappa_y * spectra[0]
    combined = jnp.concatenate([spectra, jnp.stack([spin_x, spin_y, spin_z])])
    physical = jnp.fft.ifft2(combined, axes=(-2, -1), norm="ortho").real
    x_speed, y_speed, z_speed, omega_x, omega_y, omega_z = [physical[n] for n in range(6)]
    product = jnp.stack([y_speed * omega_z - z_speed * omega_y,
                         z_speed * omega_x - x_speed * omega_z,
                         x_speed * omega_y - y_speed * omega_x])
    forcing = jnp.fft.fft2(product, axes=(-2, -1), norm="ortho")
    retained = (3 * jnp.abs(wavenumber)[:, None] < extent) & (3 * jnp.abs(wavenumber)[None, :] < extent)
    damping = jnp.exp(-viscosity * time_step * (kappa_x ** 2 + kappa_y ** 2))
    updated = damping * (spectra + time_step * jnp.where(retained, forcing, 0.0))
    velocity = jnp.stack([updated.real, updated.imag], axis=1).astype(jnp.float32)
    return velocity, jnp.swapaxes(physical[:2], -1, -2).astype(jnp.float32)


def advance(values, x_speed, y_speed):
    def neighbor(step_y, step_x):
        return jnp.roll(values, (-step_y, -step_x), axis=(1, 2))
    grad_x = (neighbor(0, -2) - neighbor(0, 2) + 8.0 * (neighbor(0, 1) - neighbor(0, -1))) / 12.0
    grad_y = (neighbor(-2, 0) - neighbor(2, 0) + 8.0 * (neighbor(1, 0) - neighbor(-1, 0))) / 12.0
    lap_x = (16.0 * (neighbor(0, 1) + neighbor(0, -1)) - neighbor(0, 2) - neighbor(0, -2) - 30.0 * values) / 12.0
    lap_y = (16.0 * (neighbor(1, 0) + neighbor(-1, 0)) - neighbor(2, 0) - neighbor(-2, 0) - 30.0 * values) / 12.0
    return values + substep * (diffusivity * (lap_x + lap_y) - (x_speed * grad_x + y_speed * grad_y))


def reference(velocity_hat, scalar, tile_offset):
    extent = velocity_hat.shape[-1]
    planes_first = jnp.moveaxis(velocity_hat, 2, 0)
    velocity_planes, speed_planes = lax.map(plane_step, planes_first)
    velocity_new = jnp.moveaxis(velocity_planes, 0, 2)
    horizontal = jnp.moveaxis(speed_planes, 0, 1)
    count = horizontal.shape[1]
    shifted = jnp.roll(horizontal, -tile_offset[0], axis=3)
    following = jnp.roll(shifted, -1, axis=3)
    refined_x = jnp.stack([shifted, (shifted + following) * 0.5], axis=4).reshape(2, count, extent, 2 * extent)
    following_y = jnp.roll(refined_x, -1, axis=2)
    refined = jnp.stack([refined_x, (refined_x + following_y) * 0.5], axis=3).reshape(2, count, 2 * extent, 2 * extent)
    halfway = advance(scalar, refined[0], refined[1])
    scalar_new = advance(halfway, refined[0], refined[1])
    return velocity_new, scalar_new
```

```python
import functools
import math

import jax
import jax.numpy as jnp
import numpy as np
from jax import lax
from jax.experimental import pallas as pl
from jax.experimental.pallas import tpu as pltpu
from jax.sharding import PartitionSpec as P

time_step = 0.25
viscosity = 2.0
diffusivity = 0.15
substep = 0.2
highest = lax.Precision.HIGHEST


def extended(cells, sides, width):
    for axis, dim in sides:
        count = lax.axis_size(axis)
        head = lax.slice_in_dim(cells, 0, width, axis=dim)
        tail = lax.slice_in_dim(cells, cells.shape[dim] - width, cells.shape[dim], axis=dim)
        cells = jnp.concatenate(
            [
                lax.ppermute(tail, axis, [(i, (i + 1) % count) for i in range(count)]),
                cells,
                lax.ppermute(head, axis, [((i + 1) % count, i) for i in range(count)]),
            ],
            axis=dim,
        )
    return cells


def dft_tables(length):
    indices = jnp.arange(length, dtype=jnp.int32)
    phases = indices[:, None] * indices[None, :] % length
    angles = phases.astype(jnp.float32) * (2.0 * math.pi / length)
    factor = 1.0 / math.sqrt(length)
    return (jnp.cos(angles) * factor, jnp.sin(angles) * factor)


def signed_wave(indices, length):
    return jnp.where(indices < length // 2, indices, indices - length)


def transpose_col(packed):
    return lax.all_to_all(packed, "col", split_axis=3, concat_axis=4, tiled=True)


def refine_rows(coarse, margin):
    current = coarse[:, :-1, :]
    following = coarse[:, 1:, :]
    paired = jnp.stack([current, (current + following) * 0.5], axis=2)
    refined = paired.reshape(coarse.shape[0], 2 * (coarse.shape[1] - 1), coarse.shape[2])
    height = 2 * (coarse.shape[1] - 2 * margin)
    return refined[:, margin : margin + height + 2 * margin, :]


def advance(values, x_speed, y_speed):
    height = values.shape[1] - 4
    breadth = values.shape[2] - 4

    def neighbor(step_y, step_x):
        return values[:, 2 + step_y : 2 + step_y + height, 2 + step_x : 2 + step_x + breadth]

    center = neighbor(0, 0)
    grad_x = (neighbor(0, -2) - neighbor(0, 2) + 8.0 * (neighbor(0, 1) - neighbor(0, -1))) / 12.0
    grad_y = (neighbor(-2, 0) - neighbor(2, 0) + 8.0 * (neighbor(1, 0) - neighbor(-1, 0))) / 12.0
    lap_x = (
        16.0 * (neighbor(0, 1) + neighbor(0, -1)) - neighbor(0, 2) - neighbor(0, -2) - 30.0 * center
    ) / 12.0
    lap_y = (
        16.0 * (neighbor(1, 0) + neighbor(-1, 0)) - neighbor(2, 0) - neighbor(-2, 0) - 30.0 * center
    ) / 12.0
    return center + substep * (
        diffusivity * (lap_x + lap_y) - (x_speed * grad_x + y_speed * grad_y)
    )


def per_device(velocity_hat, scalar, tile_offset):
    extent = velocity_hat.shape[4]
    kx_block = velocity_hat.shape[3]
    cosine_table, sine_table = dft_tables(extent)
    wave_all = signed_wave(jnp.arange(extent, dtype=jnp.int32), extent)
    local_wave = signed_wave(
        lax.axis_index("col") * kx_block + jnp.arange(kx_block, dtype=jnp.int32), extent
    )
    kappa_y = (wave_all.astype(jnp.float32) / (extent // 2))[None, None, :]
    kappa_x = (local_wave.astype(jnp.float32) / (extent // 2))[None, :, None]
    real_part = velocity_hat[:, 0]
    imag_part = velocity_hat[:, 1]
    spin_x_real = -kappa_y * imag_part[2]
    spin_x_imag = kappa_y * real_part[2]
    spin_z_real = kappa_y * imag_part[0] - kappa_x * imag_part[1]
    spin_z_imag = kappa_x * real_part[1] - kappa_y * real_part[0]
    fields_real = jnp.concatenate([real_part, jnp.stack([spin_x_real, spin_z_real])])
    fields_imag = jnp.concatenate([imag_part, jnp.stack([spin_x_imag, spin_z_imag])])
    lines_real = jnp.einsum(
        "fpkq,qy->fpyk", fields_real, cosine_table, precision=highest
    ) - jnp.einsum("fpkq,qy->fpyk", fields_imag, sine_table, precision=highest)
    lines_imag = jnp.einsum(
        "fpkq,qy->fpyk", fields_real, sine_table, precision=highest
    ) + jnp.einsum("fpkq,qy->fpyk", fields_imag, cosine_table, precision=highest)
    landed = transpose_col(jnp.stack([lines_real, lines_imag], axis=1))
    landed_real = landed[:, 0]
    landed_imag = landed[:, 1]
    wave_x = (wave_all.astype(jnp.float32) / (extent // 2))[None, None, :]
    spin_y_real = wave_x * landed_imag[2]
    spin_y_imag = -wave_x * landed_real[2]
    landed_real = jnp.concatenate([landed_real[:4], spin_y_real[None], landed_real[4:]])
    landed_imag = jnp.concatenate([landed_imag[:4], spin_y_imag[None], landed_imag[4:]])
    physical = jnp.einsum(
        "fpyk,kx->fpyx", landed_real, cosine_table, precision=highest
    ) - jnp.einsum("fpyk,kx->fpyx", landed_imag, sine_table, precision=highest)
    x_speed = physical[0]
    y_speed = physical[1]
    z_speed = physical[2]
    omega_x = physical[3]
    omega_y = physical[4]
    omega_z = physical[5]
    product = jnp.stack(
        [
            y_speed * omega_z - z_speed * omega_y,
            z_speed * omega_x - x_speed * omega_z,
            x_speed * omega_y - y_speed * omega_x,
        ]
    )
    rows_real = jnp.einsum("cpyx,xk->cpky", product, cosine_table, precision=highest)
    rows_imag = -jnp.einsum("cpyx,xk->cpky", product, sine_table, precision=highest)
    returned = transpose_col(jnp.stack([rows_real, rows_imag], axis=1))
    back_real = returned[:, 0]
    back_imag = returned[:, 1]
    forcing_real = jnp.einsum(
        "cpky,yq->cpkq", back_real, cosine_table, precision=highest
    ) + jnp.einsum("cpky,yq->cpkq", back_imag, sine_table, precision=highest)
    forcing_imag = jnp.einsum(
        "cpky,yq->cpkq", back_imag, cosine_table, precision=highest
    ) - jnp.einsum("cpky,yq->cpkq", back_real, sine_table, precision=highest)
    retained = (3 * jnp.abs(local_wave)[:, None] < extent) & (
        3 * jnp.abs(wave_all)[None, :] < extent
    )
    damping = jnp.exp(-viscosity * time_step * (kappa_x**2 + kappa_y**2))
    new_real = damping * (real_part + time_step * jnp.where(retained, forcing_real, 0.0))
    new_imag = damping * (imag_part + time_step * jnp.where(retained, forcing_imag, 0.0))
    velocity_new = jnp.stack([new_real, new_imag], axis=1)
    horizontal = physical[:2]
    doubled = jnp.concatenate([horizontal, horizontal], axis=3)
    shifted = lax.dynamic_slice_in_dim(doubled, tile_offset[0], extent, 3)
    following = jnp.concatenate([shifted[..., 1:], shifted[..., :1]], axis=3)
    refined_x = jnp.stack([shifted, (shifted + following) * 0.5], axis=4).reshape(
        2, shifted.shape[1], shifted.shape[2], 2 * extent
    )
    arrived = lax.all_to_all(refined_x, "row", split_axis=3, concat_axis=1, tiled=True)
    scalar_ext, x_coarse, y_coarse = (
        extended(scalar, (("row", 2), ("col", 1)), 2),
        extended(arrived[0], (("row", 2), ("col", 1)), 2),
        extended(arrived[1], (("row", 2), ("col", 1)), 2),
    )
    x_refined = refine_rows(x_coarse, 2)[:, 2:-2, 2:-2]
    y_refined = refine_rows(y_coarse, 2)[:, 2:-2, 2:-2]
    halfway = advance(scalar_ext, x_refined, y_refined)
    halfway_ext = extended(halfway, (("row", 2), ("col", 1)), 2)
    scalar_new = advance(halfway_ext, x_refined, y_refined)
    return (velocity_new, scalar_new)


def split(values):
    high = values.astype(jnp.bfloat16)
    return high, (values - high.astype(jnp.float32)).astype(jnp.bfloat16)


def host_split(table):
    table = table.astype(np.float32)
    high = table.astype(jnp.bfloat16)
    return high, (table - high.astype(np.float32)).astype(jnp.bfloat16)


def host_angles(rows, columns, length):
    phases = np.outer(rows, columns) % length
    return phases * (2.0 * np.pi / length)


def y_table(length):
    indices = np.arange(length)
    angles = host_angles(indices, indices, length)
    return host_split(np.concatenate([np.cos(angles), np.sin(angles)], axis=1) / np.sqrt(length))


def x_table(length, block):
    indices = np.arange(length)
    angles = host_angles(indices, indices, length).reshape(length // block, block, length)
    return host_split(
        np.stack([np.cos(angles), -np.sin(angles)], axis=1).reshape(2 * length, length)
        / np.sqrt(length)
    )


def row_weights(lines, height, next_at, last_at):
    weights = np.zeros((height + 8, lines + 8), np.float32)
    place = {**{j: j for j in range(lines)}, lines: next_at, lines + 1: next_at + 1, -1: last_at}
    for fine in range(-2, height + 2):
        base = fine // 2
        row = fine if fine >= 0 else height + 8 + fine
        if fine % 2 == 0:
            weights[row, place[base]] += 1.0
        else:
            weights[row, place[base]] += 0.5
            weights[row, place[base + 1]] += 0.5
    return weights.astype(jnp.bfloat16)


def column_weights(points, columns, breadth, total):
    weights = np.zeros((columns, total), np.float32)
    for fine in range(-2, breadth + 2):
        base = fine // 2
        at = fine if fine >= 0 else total + fine
        if fine % 2 == 0:
            weights[base + 1, at] += 1.0
        else:
            weights[base + 1, at] += 0.5
            weights[base + 2, at] += 0.5
    return weights.astype(jnp.bfloat16)


def dot(left, right, contract):
    return lax.dot_general(
        left, right, (contract, ((), ())), preferred_element_type=jnp.float32
    )


def dot3(left, right, contract):
    return (
        dot(left[0], right[0], contract)
        + dot(left[0], right[1], contract)
        + dot(left[1], right[0], contract)
    )


def lane_wave(shape, dim, start, length):
    wave = lax.broadcasted_iota(jnp.int32, shape, dim) + start
    return jnp.where(wave < length // 2, wave, wave - length)


def inverse_y(count, block, length, place, spectra, head, tail, table_high, table_low, *rest):
    outs, (spectra_high, spectra_low, lines) = rest[:count], rest[count:]
    col = place[0]
    kappa_y = lane_wave((block, length), 1, 0, length).astype(jnp.float32) / (length // 2)
    kappa_x = lane_wave((block, length), 0, col * block, length).astype(jnp.float32) / (length // 2)
    real = [spectra[f, 0, 0] for f in range(3)]
    imag = [spectra[f, 1, 0] for f in range(3)]
    real.append(-kappa_y * imag[2])
    imag.append(kappa_y * real[2])
    real.append(kappa_y * imag[0] - kappa_x * imag[1])
    imag.append(kappa_x * real[1] - kappa_y * real[0])
    for f in range(5):
        real_pair = split(real[f])
        imag_pair = split(imag[f])
        top = slice(2 * f * block, (2 * f + 1) * block)
        bottom = slice((2 * f + 1) * block, (2 * f + 2) * block)
        for store, re, im in (
            (spectra_high, real_pair[0], imag_pair[0]),
            (spectra_low, real_pair[1], imag_pair[1]),
        ):
            store[top, :length] = re
            store[top, length:] = -im
            store[bottom, :length] = im
            store[bottom, length:] = re
    lines[...] = dot3(
        (table_high[...], table_low[...]), (spectra_high[...], spectra_low[...]), ((1,), (1,))
    )
    wide = 2 * block
    sub = lax.broadcasted_iota(jnp.int32, (8, wide), 0)
    for s in range(count):
        dest = lax.rem(col + s, count)
        base = pl.multiple_of(dest * block, 8)
        for f in range(5):
            outs[s][f * block : (f + 1) * block, :] = lines[
                pl.ds(base, block), f * wide : (f + 1) * wide
            ]
        following = pl.multiple_of(lax.rem(dest + 1, count) * block, 8)
        before = pl.multiple_of(lax.rem(dest + count - 1, count) * block + block - 8, 8)
        next_x = lines[pl.ds(following, 8), 0:wide]
        next_y = pltpu.roll(lines[pl.ds(following, 8), wide : 2 * wide], 2, 0)
        last_x = lines[pl.ds(before, 8), 0:wide]
        last_y = pltpu.roll(lines[pl.ds(before, 8), wide : 2 * wide], 7, 0)
        rim = jnp.where(sub < 2, next_x, jnp.where(sub < 4, next_y, jnp.where(sub < 7, last_y, last_x)))
        at = 5 * block
        outs[s][at : at + 8, :] = rim
        at += 8
        edges = ([tail] if s == 1 else []) + ([head] if s == count - 1 else [])
        for edge in edges:
            for p in range(edge.shape[0]):
                for b in range(edge.shape[2] // wide):
                    outs[s][at : at + 8, :] = edge[p, :, b * wide : (b + 1) * wide]
                    at += 8


def middle(count, rows, block, length, planes, breadth, place, *refs):
    slabs = refs[:count]
    first, final, table_high, table_low = refs[count : count + 4]
    outs = refs[count + 4 : 2 * count + 4]
    windows = refs[2 * count + 4 : 2 * count + 4 + rows]
    rim_out, lhs_high, lhs_low, freq = refs[2 * count + 4 + rows :]
    col, row, offset = place[0], place[1], place[2]
    wide = 2 * block
    lane = lax.broadcasted_iota(jnp.int32, (1, wide), 1)
    for s in range(count):
        source = lax.rem(col + count - s, count)
        at = pl.multiple_of(source * wide, wide)
        value = slabs[s][0 : 5 * block, :]
        high, low = split(value)
        lhs_high[0 : 5 * block, pl.ds(at, wide)] = high
        lhs_low[0 : 5 * block, pl.ds(at, wide)] = low
        wave = lax.rem(lane, block) + source * block
        wave = jnp.where(wave < length // 2, wave, wave - length)
        kappa = wave.astype(jnp.float32) / (length // 2)
        kappa = jnp.where(lane < block, kappa, -kappa)
        spin = jnp.concatenate(
            [
                pltpu.roll(value[2 * block : 3 * block], block, 1) * kappa,
                slabs[s][5 * block : 5 * block + 8, :],
                jnp.zeros((8, wide), jnp.float32),
            ]
        )
        high, low = split(spin)
        lhs_high[5 * block :, pl.ds(at, wide)] = high
        lhs_low[5 * block :, pl.ds(at, wide)] = low
    table = (table_high[...], table_low[...])
    physical = dot3((lhs_high[...], lhs_low[...]), table, ((1,), (0,)))
    u, v, w, spin_x, spin_z, spin_y = [physical[f * block : (f + 1) * block] for f in range(6)]
    product = jnp.concatenate([v * spin_z - w * spin_y, w * spin_x - u * spin_z, u * spin_y - v * spin_x])
    freq[...] = dot3(split(product), table, ((1,), (1,)))
    for s in range(count):
        at = pl.multiple_of(lax.rem(col + s, count) * wide, wide)
        outs[s][...] = freq[:, pl.ds(at, wide)]
    rim = physical[6 * block : 6 * block + 8]
    sub = lax.broadcasted_iota(jnp.int32, (8, wide), 0)
    pieces = breadth // wide
    edge = 5 * block + 8
    top_at = edge
    bottom_at = edge if count > 2 else edge + 8 * planes * pieces
    if count == 1:
        raise ValueError("one column")
    for p in range(planes):
        for b in range(pieces):
            step = 8 * (p * pieces + b)
            upper = slabs[1][top_at + step : top_at + step + 8, :]
            lower = slabs[count - 1][bottom_at + step : bottom_at + step + 8, :]
            rim_out[p, :, b * wide : (b + 1) * wide] = jnp.where(sub < 4, lower, upper)
    cells = breadth // 2
    height = first.shape[1]
    kept = windows[0].shape[0] - planes * (height + 8)
    lines = block + 8
    span = kept // (2 * lines)
    for s in range(rows):
        target = lax.rem(row + s, rows)
        shift = lax.rem(2 * length + 1 - offset - target * cells, length)
        for f, field in enumerate((u, v)):
            rolled = pltpu.roll(jnp.concatenate([field, rim]), shift, 1)
            for b in range(span):
                at = (f * span + b) * lines
                windows[s][at : at + lines, :] = rolled[:, b * wide : (b + 1) * wide]
        if s > 0:
            for p in range(planes):
                at = kept + p * (height + 8)
                windows[s][at : at + height, :] = jnp.where(lane < block, first[p], final[p])
                windows[s][at + height : at + height + 8, :] = jnp.where(
                    lane < block, rim_out[p, :, 0:wide], rim_out[p, :, breadth - wide : breadth]
                )


def transport(rows, block, planes, place, *refs):
    scalar, rim = refs[0], refs[1]
    windows = refs[2 : 2 + rows]
    weights_x, weights_y, across, out = refs[2 + rows :]
    row = place[1]
    wide = 2 * block
    height, breadth = scalar.shape[1], scalar.shape[2]
    lines = block + 8
    kept = windows[0].shape[0] - planes * (height + 8)
    span = kept // (2 * lines)
    lane = lax.broadcasted_iota(jnp.int32, (1, wide), 1)
    per_row = planes // rows
    tall, total = height + 8, breadth + wide

    def shifted(values, amount, axis):
        return pltpu.roll(values, (-amount) % values.shape[axis], axis)

    for s in range(rows):
        source = lax.rem(row + rows - s, rows)
        speeds = []
        for f, weights in enumerate((weights_x, weights_y)):
            coarse = jnp.concatenate(
                [windows[s][(f * span + b) * lines : (f * span + b + 1) * lines, :] for b in range(span)],
                axis=1,
            )
            high, low = split(coarse)
            taller = dot(weights[...], high, ((1,), (0,))) + dot(weights[...], low, ((1,), (0,)))
            high, low = split(taller)
            speeds.append(dot(high, across[...], ((1,), (0,))) + dot(low, across[...], ((1,), (0,))))
        x_speed, y_speed = speeds
        for q in range(per_row):
            p = source * per_row + q
            sides = []
            for part in (1 % rows, rows - 1):
                sides.append(windows[part][pl.ds(pl.multiple_of(kept + p * tall, 8), tall), :])
            values = jnp.concatenate(
                [
                    jnp.concatenate([scalar[p], rim[p]], axis=0),
                    jnp.where(lane < block, sides[1], sides[0]),
                ],
                axis=1,
            )
            for _ in range(2):
                right, left = shifted(values, 1, 1), shifted(values, -1, 1)
                right2, left2 = shifted(values, 2, 1), shifted(values, -2, 1)
                below, above = shifted(values, 1, 0), shifted(values, -1, 0)
                below2, above2 = shifted(values, 2, 0), shifted(values, -2, 0)
                grad_x = left2 - right2 + 8.0 * (right - left)
                grad_y = above2 - below2 + 8.0 * (below - above)
                near = (right + left) + (below + above)
                far = (right2 + left2) + (below2 + above2)
                spread = 16.0 * near - far - 60.0 * values
                values = values + (substep / 12.0) * (
                    diffusivity * spread - (x_speed * grad_x + y_speed * grad_y)
                )
            out[p] = values[:height, :breadth]


def forward_y(count, block, length, place, *refs):
    slabs = refs[:count]
    spectra, table_high, table_low, out, gathered = refs[count:]
    col = place[0]
    wide = 2 * block
    for s in range(count):
        source = lax.rem(col + count - s, count)
        at = pl.multiple_of(source * block, 8)
        for f in range(3):
            gathered[pl.ds(at, block), f * wide : (f + 1) * wide] = slabs[s][
                f * block : (f + 1) * block, :
            ]
    parts = dot3(split(gathered[...].T), (table_high[...], table_low[...]), ((1,), (0,)))
    wave_y = lane_wave((block, length), 1, 0, length)
    wave_x = lane_wave((block, length), 0, col * block, length)
    kappa_y = wave_y.astype(jnp.float32) / (length // 2)
    kappa_x = wave_x.astype(jnp.float32) / (length // 2)
    damping = jnp.exp(-viscosity * time_step * (kappa_x * kappa_x + kappa_y * kappa_y))
    retained = (3 * jnp.abs(wave_x) < length) & (3 * jnp.abs(wave_y) < length)
    for f in range(3):
        real = parts[f * wide : f * wide + block]
        imag = parts[f * wide + block : (f + 1) * wide]
        forcing_real = real[:, :length] + imag[:, length:]
        forcing_imag = imag[:, :length] - real[:, length:]
        out[f, 0, 0] = damping * (
            spectra[f, 0, 0] + time_step * jnp.where(retained, forcing_real, 0.0)
        )
        out[f, 1, 0] = damping * (
            spectra[f, 1, 0] + time_step * jnp.where(retained, forcing_imag, 0.0)
        )


def whole_spec(shape):
    return pl.BlockSpec(shape, lambda *_: (0,) * len(shape))


def kernel_call(body, name, operands, specs, out_shapes, scratch=()):
    return pl.pallas_call(
        body,
        name=name,
        grid=(1,),
        in_specs=[pl.BlockSpec(memory_space=pltpu.SMEM)] + specs,
        out_specs=[whole_spec(s) for s in out_shapes],
        out_shape=[jax.ShapeDtypeStruct(s, jnp.float32) for s in out_shapes],
        scratch_shapes=list(scratch),
        compiler_params=pltpu.CompilerParams(vmem_limit_bytes=60 * 1024 * 1024),
    )(*operands)


def exchange(slabs, axis):
    count = lax.axis_size(axis)
    return [slabs[0]] + [
        lax.ppermute(slabs[s], axis, [(i, (i + s) % count) for i in range(count)])
        for s in range(1, count)
    ]


def fast_device(velocity_hat, scalar, tile_offset):
    length = velocity_hat.shape[4]
    block = velocity_hat.shape[3]
    planes, height, breadth = scalar.shape
    count = lax.axis_size("col")
    rows = lax.axis_size("row")
    wide = 2 * block
    place = jnp.stack(
        [lax.axis_index("col"), lax.axis_index("row"), tile_offset[0]]
    ).astype(jnp.int32)
    y_high, y_low = [jnp.asarray(t) for t in y_table(length)]
    x_high, x_low = [jnp.asarray(t) for t in x_table(length, block)]
    y_specs = [whole_spec(y_high.shape)] * 2
    x_specs = [whole_spec(x_high.shape)] * 2
    edge_rows = 8 * planes * (breadth // wide)
    slab_rows = [
        5 * block + 8 + edge_rows * ((s == 1) + (s == count - 1)) for s in range(count)
    ]
    slabs = kernel_call(
        functools.partial(inverse_y, count, block, length),
        "inverse_y",
        [place, velocity_hat, scalar, scalar, y_high, y_low],
        [
            whole_spec(velocity_hat.shape),
            pl.BlockSpec((planes, 8, breadth), lambda *_: (0, 0, 0)),
            pl.BlockSpec((planes, 8, breadth), lambda *_: (0, height // 8 - 1, 0)),
        ]
        + y_specs,
        [(r, wide) for r in slab_rows],
        [
            pltpu.VMEM((10 * block, 2 * length), jnp.bfloat16),
            pltpu.VMEM((10 * block, 2 * length), jnp.bfloat16),
            pltpu.VMEM((length, 10 * block), jnp.float32),
        ],
    )
    slabs = exchange(slabs, "col")
    lines = block + 8
    columns = -(-(breadth // 2 + 3) // wide) * wide
    window_rows = 2 * lines * (columns // wide) + planes * (height + 8)
    results = kernel_call(
        functools.partial(middle, count, rows, block, length, planes, breadth),
        "middle",
        [place, *slabs, scalar, scalar, x_high, x_low],
        [whole_spec(s.shape) for s in slabs]
        + [
            pl.BlockSpec((planes, height, wide), lambda *_: (0, 0, 0)),
            pl.BlockSpec((planes, height, wide), lambda *_: (0, 0, breadth // wide - 1)),
        ]
        + x_specs,
        [(3 * block, wide)] * count + [(window_rows, wide)] * rows + [(planes, 8, breadth)],
        [
            pltpu.VMEM((6 * block + 16, 2 * length), jnp.bfloat16),
            pltpu.VMEM((6 * block + 16, 2 * length), jnp.bfloat16),
            pltpu.VMEM((3 * block, 2 * length), jnp.float32),
        ],
    )
    windows = exchange(results[count : count + rows], "row")
    returned = exchange(results[:count], "col")
    rim = results[count + rows]
    weights = [
        jnp.asarray(row_weights(block, height, block, block + 7)),
        jnp.asarray(row_weights(block, height, block + 2, block + 6)),
        jnp.asarray(column_weights(breadth // 2, columns, breadth, breadth + wide)),
    ]
    (scalar_new,) = kernel_call(
        functools.partial(transport, rows, block, planes),
        "transport",
        [place, scalar, rim, *windows, *weights],
        [whole_spec(x.shape) for x in (scalar, rim, *windows, *weights)],
        [scalar.shape],
    )
    (velocity_new,) = kernel_call(
        functools.partial(forward_y, count, block, length),
        "forward_y",
        [place, *returned, velocity_hat, y_high, y_low],
        [whole_spec(x.shape) for x in (*returned, velocity_hat)] + y_specs,
        [velocity_hat.shape],
        [pltpu.VMEM((length, 3 * wide), jnp.float32)],
    )
    return velocity_new, scalar_new


def fits(mesh, velocity_hat, scalar):
    count, rows = mesh.shape["col"], mesh.shape["row"]
    planes = velocity_hat.shape[2] // (mesh.shape["group"] * rows)
    length = velocity_hat.shape[4]
    block = velocity_hat.shape[3] // count
    height, breadth = scalar.shape[1] // count, scalar.shape[2] // rows
    return (
        planes == 1
        and 2 < count <= 8
        and 1 < rows <= 8
        and (2 * block) % 128 == 0
        and height == 2 * block
        and breadth * rows == 2 * length
        and breadth % (2 * block) == 0
        and breadth // 2 + 3 <= length
    )


def solution(mesh):
    def step(velocity_hat, scalar, tile_offset):
        body = fast_device if fits(mesh, velocity_hat, scalar) else per_device
        return jax.shard_map(
            body,
            mesh=mesh,
            in_specs=(P(None, None, ("group", "row"), "col", None), P("group", "col", "row"), P()),
            out_specs=(P(None, None, ("group", "row"), "col", None), P("group", "col", "row")),
            check_vma=False,
        )(velocity_hat, scalar, tile_offset)

    return step
```

```python
import functools
import itertools
import math

import jax
import jax.numpy as jnp
import numpy as np
from jax import lax
from jax.experimental import pallas as pl
from jax.experimental.pallas import tpu as pltpu
from jax.sharding import PartitionSpec as P


time_step = 0.25
viscosity = 2.0
diffusivity = 0.15
substep = 0.2
highest = lax.Precision.HIGHEST


def extended(cells, sides, width):
    for axis, dim in sides:
        count = lax.axis_size(axis)
        head = lax.slice_in_dim(cells, 0, width, axis=dim)
        tail = lax.slice_in_dim(cells, cells.shape[dim] - width, cells.shape[dim], axis=dim)
        cells = jnp.concatenate(
            [
                lax.ppermute(tail, axis, [(i, (i + 1) % count) for i in range(count)]),
                cells,
                lax.ppermute(head, axis, [((i + 1) % count, i) for i in range(count)]),
            ],
            axis=dim,
        )
    return cells


def dft_tables(length):
    indices = jnp.arange(length, dtype=jnp.int32)
    phases = indices[:, None] * indices[None, :] % length
    angles = phases.astype(jnp.float32) * (2.0 * math.pi / length)
    factor = 1.0 / math.sqrt(length)
    return (jnp.cos(angles) * factor, jnp.sin(angles) * factor)


def signed_wave(indices, length):
    return jnp.where(indices < length // 2, indices, indices - length)


def transpose_col(packed):
    return lax.all_to_all(packed, "col", split_axis=3, concat_axis=4, tiled=True)


def refine_rows(coarse, margin):
    current = coarse[:, :-1, :]
    following = coarse[:, 1:, :]
    paired = jnp.stack([current, (current + following) * 0.5], axis=2)
    refined = paired.reshape(coarse.shape[0], 2 * (coarse.shape[1] - 1), coarse.shape[2])
    height = 2 * (coarse.shape[1] - 2 * margin)
    return refined[:, margin : margin + height + 2 * margin, :]


def advance(values, x_speed, y_speed):
    height = values.shape[1] - 4
    breadth = values.shape[2] - 4

    def neighbor(step_y, step_x):
        return values[:, 2 + step_y : 2 + step_y + height, 2 + step_x : 2 + step_x + breadth]

    center = neighbor(0, 0)
    grad_x = (neighbor(0, -2) - neighbor(0, 2) + 8.0 * (neighbor(0, 1) - neighbor(0, -1))) / 12.0
    grad_y = (neighbor(-2, 0) - neighbor(2, 0) + 8.0 * (neighbor(1, 0) - neighbor(-1, 0))) / 12.0
    lap_x = (
        16.0 * (neighbor(0, 1) + neighbor(0, -1)) - neighbor(0, 2) - neighbor(0, -2) - 30.0 * center
    ) / 12.0
    lap_y = (
        16.0 * (neighbor(1, 0) + neighbor(-1, 0)) - neighbor(2, 0) - neighbor(-2, 0) - 30.0 * center
    ) / 12.0
    return center + substep * (
        diffusivity * (lap_x + lap_y) - (x_speed * grad_x + y_speed * grad_y)
    )


def per_device(velocity_hat, scalar, tile_offset):
    extent = velocity_hat.shape[4]
    kx_block = velocity_hat.shape[3]
    cosine_table, sine_table = dft_tables(extent)
    wave_all = signed_wave(jnp.arange(extent, dtype=jnp.int32), extent)
    local_wave = signed_wave(
        lax.axis_index("col") * kx_block + jnp.arange(kx_block, dtype=jnp.int32), extent
    )
    kappa_y = (wave_all.astype(jnp.float32) / (extent // 2))[None, None, :]
    kappa_x = (local_wave.astype(jnp.float32) / (extent // 2))[None, :, None]
    real_part = velocity_hat[:, 0]
    imag_part = velocity_hat[:, 1]
    spin_x_real = -kappa_y * imag_part[2]
    spin_x_imag = kappa_y * real_part[2]
    spin_z_real = kappa_y * imag_part[0] - kappa_x * imag_part[1]
    spin_z_imag = kappa_x * real_part[1] - kappa_y * real_part[0]
    fields_real = jnp.concatenate([real_part, jnp.stack([spin_x_real, spin_z_real])])
    fields_imag = jnp.concatenate([imag_part, jnp.stack([spin_x_imag, spin_z_imag])])
    lines_real = jnp.einsum(
        "fpkq,qy->fpyk", fields_real, cosine_table, precision=highest
    ) - jnp.einsum("fpkq,qy->fpyk", fields_imag, sine_table, precision=highest)
    lines_imag = jnp.einsum(
        "fpkq,qy->fpyk", fields_real, sine_table, precision=highest
    ) + jnp.einsum("fpkq,qy->fpyk", fields_imag, cosine_table, precision=highest)
    landed = transpose_col(jnp.stack([lines_real, lines_imag], axis=1))
    landed_real = landed[:, 0]
    landed_imag = landed[:, 1]
    wave_x = (wave_all.astype(jnp.float32) / (extent // 2))[None, None, :]
    spin_y_real = wave_x * landed_imag[2]
    spin_y_imag = -wave_x * landed_real[2]
    landed_real = jnp.concatenate([landed_real[:4], spin_y_real[None], landed_real[4:]])
    landed_imag = jnp.concatenate([landed_imag[:4], spin_y_imag[None], landed_imag[4:]])
    physical = jnp.einsum(
        "fpyk,kx->fpyx", landed_real, cosine_table, precision=highest
    ) - jnp.einsum("fpyk,kx->fpyx", landed_imag, sine_table, precision=highest)
    x_speed = physical[0]
    y_speed = physical[1]
    z_speed = physical[2]
    omega_x = physical[3]
    omega_y = physical[4]
    omega_z = physical[5]
    product = jnp.stack(
        [
            y_speed * omega_z - z_speed * omega_y,
            z_speed * omega_x - x_speed * omega_z,
            x_speed * omega_y - y_speed * omega_x,
        ]
    )
    rows_real = jnp.einsum("cpyx,xk->cpky", product, cosine_table, precision=highest)
    rows_imag = -jnp.einsum("cpyx,xk->cpky", product, sine_table, precision=highest)
    returned = transpose_col(jnp.stack([rows_real, rows_imag], axis=1))
    back_real = returned[:, 0]
    back_imag = returned[:, 1]
    forcing_real = jnp.einsum(
        "cpky,yq->cpkq", back_real, cosine_table, precision=highest
    ) + jnp.einsum("cpky,yq->cpkq", back_imag, sine_table, precision=highest)
    forcing_imag = jnp.einsum(
        "cpky,yq->cpkq", back_imag, cosine_table, precision=highest
    ) - jnp.einsum("cpky,yq->cpkq", back_real, sine_table, precision=highest)
    retained = (3 * jnp.abs(local_wave)[:, None] < extent) & (
        3 * jnp.abs(wave_all)[None, :] < extent
    )
    damping = jnp.exp(-viscosity * time_step * (kappa_x**2 + kappa_y**2))
    new_real = damping * (real_part + time_step * jnp.where(retained, forcing_real, 0.0))
    new_imag = damping * (imag_part + time_step * jnp.where(retained, forcing_imag, 0.0))
    velocity_new = jnp.stack([new_real, new_imag], axis=1)
    horizontal = physical[:2]
    doubled = jnp.concatenate([horizontal, horizontal], axis=3)
    shifted = lax.dynamic_slice_in_dim(doubled, tile_offset[0], extent, 3)
    following = jnp.concatenate([shifted[..., 1:], shifted[..., :1]], axis=3)
    refined_x = jnp.stack([shifted, (shifted + following) * 0.5], axis=4).reshape(
        2, shifted.shape[1], shifted.shape[2], 2 * extent
    )
    arrived = lax.all_to_all(refined_x, "row", split_axis=3, concat_axis=1, tiled=True)
    scalar_ext, x_coarse, y_coarse = (
        extended(scalar, (("row", 2), ("col", 1)), 2),
        extended(arrived[0], (("row", 2), ("col", 1)), 2),
        extended(arrived[1], (("row", 2), ("col", 1)), 2),
    )
    x_refined = refine_rows(x_coarse, 2)[:, 2:-2, 2:-2]
    y_refined = refine_rows(y_coarse, 2)[:, 2:-2, 2:-2]
    halfway = advance(scalar_ext, x_refined, y_refined)
    halfway_ext = extended(halfway, (("row", 2), ("col", 1)), 2)
    scalar_new = advance(halfway_ext, x_refined, y_refined)
    return (velocity_new, scalar_new)


def split(values):
    high = values.astype(jnp.bfloat16)
    return high, (values - high.astype(jnp.float32)).astype(jnp.bfloat16)


def host_split(table):
    table = table.astype(np.float32)
    high = table.astype(jnp.bfloat16)
    return high, (table - high.astype(np.float32)).astype(jnp.bfloat16)


def host_angles(rows, columns, length):
    phases = np.outer(rows, columns) % length
    return phases * (2.0 * np.pi / length)


def y_table(length):
    indices = np.arange(length)
    angles = host_angles(indices, indices, length)
    return host_split(np.concatenate([np.cos(angles), np.sin(angles)], axis=1) / np.sqrt(length))


def x_table(length, block):
    indices = np.arange(length)
    angles = host_angles(indices, indices, length).reshape(length // block, block, length)
    return host_split(
        np.stack([np.cos(angles), -np.sin(angles)], axis=1).reshape(2 * length, length)
        / np.sqrt(length)
    )


def row_weights(lines, height, next_at, last_at):
    weights = np.zeros((height + 8, lines + 8), np.float32)
    place = {**{j: j for j in range(lines)}, lines: next_at, lines + 1: next_at + 1, -1: last_at}
    for fine in range(-2, height + 2):
        base = fine // 2
        row = fine if fine >= 0 else height + 8 + fine
        if fine % 2 == 0:
            weights[row, place[base]] += 1.0
        else:
            weights[row, place[base]] += 0.5
            weights[row, place[base + 1]] += 0.5
    return weights.astype(jnp.bfloat16)


def column_weights(columns, breadth, total):
    weights = np.zeros((columns, total), np.float32)
    for fine in range(-2, breadth + 2):
        base = fine // 2
        at = fine if fine >= 0 else total + fine
        if fine % 2 == 0:
            weights[base + 1, at] += 1.0
        else:
            weights[base + 1, at] += 0.5
            weights[base + 2, at] += 0.5
    return weights.astype(jnp.bfloat16)


def dot(left, right, contract):
    return lax.dot_general(
        left, right, (contract, ((), ())), preferred_element_type=jnp.float32
    )


def dot3(left, right, contract):
    return (
        dot(left[0], right[0], contract)
        + dot(left[0], right[1], contract)
        + dot(left[1], right[0], contract)
    )


def lane_wave(shape, dim, start, length):
    wave = lax.broadcasted_iota(jnp.int32, shape, dim) + start
    return jnp.where(wave < length // 2, wave, wave - length)


def inverse_y(count, block, length, routes, near, spectra, head, tail, table_high, table_low, *rest):
    outs, (spectra_high, spectra_low, lines) = rest[:count], rest[count:]
    col = lax.axis_index("col")
    kappa_y = lane_wave((block, length), 1, 0, length).astype(jnp.float32) / (length // 2)
    kappa_x = lane_wave((block, length), 0, col * block, length).astype(jnp.float32) / (length // 2)
    real = [spectra[f, 0, 0] for f in range(3)]
    imag = [spectra[f, 1, 0] for f in range(3)]
    real.append(-kappa_y * imag[2])
    imag.append(kappa_y * real[2])
    real.append(kappa_y * imag[0] - kappa_x * imag[1])
    imag.append(kappa_x * real[1] - kappa_y * real[0])
    for f in range(5):
        real_pair = split(real[f])
        imag_pair = split(imag[f])
        top = slice(2 * f * block, (2 * f + 1) * block)
        bottom = slice((2 * f + 1) * block, (2 * f + 2) * block)
        for store, re, im in (
            (spectra_high, real_pair[0], imag_pair[0]),
            (spectra_low, real_pair[1], imag_pair[1]),
        ):
            store[top, :length] = re
            store[top, length:] = -im
            store[bottom, :length] = im
            store[bottom, length:] = re
    lines[...] = dot3(
        (table_high[...], table_low[...]), (spectra_high[...], spectra_low[...]), ((1,), (1,))
    )
    wide = 2 * block
    sub = lax.broadcasted_iota(jnp.int32, (8, wide), 0)
    for s in range(count):
        dest = routes[0, s, col]
        base = pl.multiple_of(dest * block, 8)
        for f in range(5):
            outs[s][f * block : (f + 1) * block, :] = lines[
                pl.ds(base, block), f * wide : (f + 1) * wide
            ]
        following = pl.multiple_of(lax.rem(dest + 1, count) * block, 8)
        before = pl.multiple_of(lax.rem(dest + count - 1, count) * block + block - 8, 8)
        next_x = lines[pl.ds(following, 8), 0:wide]
        next_y = pltpu.roll(lines[pl.ds(following, 8), wide : 2 * wide], 2, 0)
        last_x = lines[pl.ds(before, 8), 0:wide]
        last_y = pltpu.roll(lines[pl.ds(before, 8), wide : 2 * wide], 7, 0)
        rim = jnp.where(sub < 2, next_x, jnp.where(sub < 4, next_y, jnp.where(sub < 7, last_y, last_x)))
        at = 5 * block
        outs[s][at : at + 8, :] = rim
        at += 8
        edges = ([tail] if s == near[0] else []) + ([head] if s == near[1] else [])
        for edge in edges:
            for p in range(edge.shape[0]):
                for b in range(edge.shape[2] // wide):
                    outs[s][at : at + 8, :] = edge[p, :, b * wide : (b + 1) * wide]
                    at += 8


def middle(count, rows, block, length, planes, breadth, near, offsets, arrivals, departures, *refs):
    slabs = refs[:count]
    first, final, table_high, table_low = refs[count : count + 4]
    outs = refs[count + 4 : 2 * count + 4]
    windows = refs[2 * count + 4 : 2 * count + 4 + rows]
    rim_out, lhs_high, lhs_low, freq = refs[2 * count + 4 + rows :]
    col, row, offset = lax.axis_index("col"), lax.axis_index("row"), offsets[0]
    wide = 2 * block
    lane = lax.broadcasted_iota(jnp.int32, (1, wide), 1)
    for s in range(count):
        source = arrivals[1, s, col]
        at = pl.multiple_of(source * wide, wide)
        value = slabs[s][0 : 5 * block, :]
        high, low = split(value)
        lhs_high[0 : 5 * block, pl.ds(at, wide)] = high
        lhs_low[0 : 5 * block, pl.ds(at, wide)] = low
        wave = lax.rem(lane, block) + source * block
        wave = jnp.where(wave < length // 2, wave, wave - length)
        kappa = wave.astype(jnp.float32) / (length // 2)
        kappa = jnp.where(lane < block, kappa, -kappa)
        spin = jnp.concatenate(
            [
                pltpu.roll(value[2 * block : 3 * block], block, 1) * kappa,
                slabs[s][5 * block : 5 * block + 8, :],
                jnp.zeros((8, wide), jnp.float32),
            ]
        )
        high, low = split(spin)
        lhs_high[5 * block :, pl.ds(at, wide)] = high
        lhs_low[5 * block :, pl.ds(at, wide)] = low
    table = (table_high[...], table_low[...])
    physical = dot3((lhs_high[...], lhs_low[...]), table, ((1,), (0,)))
    u, v, w, spin_x, spin_z, spin_y = [physical[f * block : (f + 1) * block] for f in range(6)]
    product = jnp.concatenate([v * spin_z - w * spin_y, w * spin_x - u * spin_z, u * spin_y - v * spin_x])
    freq[...] = dot3(split(product), table, ((1,), (1,)))
    for s in range(count):
        at = pl.multiple_of(departures[0, s, col] * wide, wide)
        outs[s][...] = freq[:, pl.ds(at, wide)]
    rim = physical[6 * block : 6 * block + 8]
    sub = lax.broadcasted_iota(jnp.int32, (8, wide), 0)
    pieces = breadth // wide
    edge = 5 * block + 8
    for p in range(planes):
        for b in range(pieces):
            step = 8 * (p * pieces + b)
            upper = slabs[near[0]][edge + step : edge + step + 8, :]
            lower = slabs[near[1]][edge + step : edge + step + 8, :]
            rim_out[p, :, b * wide : (b + 1) * wide] = jnp.where(sub < 4, lower, upper)
    cells = breadth // 2
    height = first.shape[1]
    kept = windows[0].shape[0] - planes * (height + 8)
    lines = block + 8
    span = kept // (2 * lines)
    for s in range(rows):
        target = lax.rem(row + s, rows)
        shift = lax.rem(2 * length + 1 - offset - target * cells, length)
        for f, field in enumerate((u, v)):
            rolled = pltpu.roll(jnp.concatenate([field, rim]), shift, 1)
            for b in range(span):
                at = (f * span + b) * lines
                windows[s][at : at + lines, :] = rolled[:, b * wide : (b + 1) * wide]
        if s > 0:
            for p in range(planes):
                at = kept + p * (height + 8)
                windows[s][at : at + height, :] = jnp.where(lane < block, first[p], final[p])
                windows[s][at + height : at + height + 8, :] = jnp.where(
                    lane < block, rim_out[p, :, 0:wide], rim_out[p, :, breadth - wide : breadth]
                )


def transport(rows, block, planes, *refs):
    scalar, rim = refs[0], refs[1]
    windows = refs[2 : 2 + rows]
    weights_x, weights_y, across, out = refs[2 + rows :]
    row = lax.axis_index("row")
    wide = 2 * block
    height, breadth = scalar.shape[1], scalar.shape[2]
    lines = block + 8
    kept = windows[0].shape[0] - planes * (height + 8)
    span = kept // (2 * lines)
    lane = lax.broadcasted_iota(jnp.int32, (1, wide), 1)
    per_row = planes // rows
    tall = height + 8

    def shifted(values, amount, axis):
        return pltpu.roll(values, (-amount) % values.shape[axis], axis)

    for s in range(rows):
        source = lax.rem(row + rows - s, rows)
        speeds = []
        for f, weights in enumerate((weights_x, weights_y)):
            coarse = jnp.concatenate(
                [windows[s][(f * span + b) * lines : (f * span + b + 1) * lines, :] for b in range(span)],
                axis=1,
            )
            high, low = split(coarse)
            taller = dot(weights[...], high, ((1,), (0,))) + dot(weights[...], low, ((1,), (0,)))
            high, low = split(taller)
            speeds.append(dot(high, across[...], ((1,), (0,))) + dot(low, across[...], ((1,), (0,))))
        x_speed, y_speed = speeds
        for q in range(per_row):
            p = source * per_row + q
            sides = []
            for part in (1 % rows, rows - 1):
                sides.append(windows[part][pl.ds(pl.multiple_of(kept + p * tall, 8), tall), :])
            values = jnp.concatenate(
                [
                    jnp.concatenate([scalar[p], rim[p]], axis=0),
                    jnp.where(lane < block, sides[1], sides[0]),
                ],
                axis=1,
            )
            for _ in range(2):
                right, left = shifted(values, 1, 1), shifted(values, -1, 1)
                right2, left2 = shifted(values, 2, 1), shifted(values, -2, 1)
                below, above = shifted(values, 1, 0), shifted(values, -1, 0)
                below2, above2 = shifted(values, 2, 0), shifted(values, -2, 0)
                grad_x = left2 - right2 + 8.0 * (right - left)
                grad_y = above2 - below2 + 8.0 * (below - above)
                near = (right + left) + (below + above)
                far = (right2 + left2) + (below2 + above2)
                spread = 16.0 * near - far - 60.0 * values
                values = values + (substep / 12.0) * (
                    diffusivity * spread - (x_speed * grad_x + y_speed * grad_y)
                )
            out[p] = values[:height, :breadth]


def forward_y(count, block, length, departures, *refs):
    slabs = refs[:count]
    spectra, table_high, table_low, out, gathered = refs[count:]
    col = lax.axis_index("col")
    wide = 2 * block
    for s in range(count):
        source = departures[1, s, col]
        at = pl.multiple_of(source * block, 8)
        for f in range(3):
            gathered[pl.ds(at, block), f * wide : (f + 1) * wide] = slabs[s][
                f * block : (f + 1) * block, :
            ]
    parts = dot3(split(gathered[...].T), (table_high[...], table_low[...]), ((1,), (0,)))
    wave_y = lane_wave((block, length), 1, 0, length)
    wave_x = lane_wave((block, length), 0, col * block, length)
    kappa_y = wave_y.astype(jnp.float32) / (length // 2)
    kappa_x = wave_x.astype(jnp.float32) / (length // 2)
    damping = jnp.exp(-viscosity * time_step * (kappa_x * kappa_x + kappa_y * kappa_y))
    retained = (3 * jnp.abs(wave_x) < length) & (3 * jnp.abs(wave_y) < length)
    for f in range(3):
        real = parts[f * wide : f * wide + block]
        imag = parts[f * wide + block : (f + 1) * wide]
        forcing_real = real[:, :length] + imag[:, length:]
        forcing_imag = imag[:, :length] - real[:, length:]
        out[f, 0, 0] = damping * (
            spectra[f, 0, 0] + time_step * jnp.where(retained, forcing_real, 0.0)
        )
        out[f, 1, 0] = damping * (
            spectra[f, 1, 0] + time_step * jnp.where(retained, forcing_imag, 0.0)
        )


def whole_spec(shape):
    return pl.BlockSpec(shape, lambda *_: (0,) * len(shape))


def kernel_call(body, scalars, operands, specs, out_shapes, scratch=(), cost=None):
    return pl.pallas_call(
        body,
        grid=(1,),
        in_specs=[pl.BlockSpec(memory_space=pltpu.SMEM)] * len(scalars) + specs,
        out_specs=[whole_spec(s) for s in out_shapes],
        out_shape=[jax.ShapeDtypeStruct(s, jnp.float32) for s in out_shapes],
        scratch_shapes=list(scratch),
        compiler_params=pltpu.CompilerParams(vmem_limit_bytes=20 * 1024 * 1024),
        cost_estimate=cost,
    )(*scalars, *operands)


def shift_routes(count):
    order = sorted(range(1, count), key=lambda s: (-min(s, count - s), s))
    return [tuple((i + s) % count for i in range(count)) for s in order]


def needed_routes(count, needed):
    pairs = [[int(needed[d] and i != d) for d in range(count)] for i in range(count)]
    spare = [i for i in range(count) for _ in range(count - 1 - sum(pairs[i]))]
    idle = [d for d in range(count) if not needed[d] for _ in range(count - 1)]
    for i, d in zip(spare, idle):
        pairs[i][d] += 1
    far = [[2 * abs(i - d) if needed[d] else 0 for d in range(count)] for i in range(count)]
    routes = []
    for _ in range(count - 1):
        best = max(
            (
                p
                for p in itertools.permutations(range(count))
                if all(pairs[i][p[i]] for i in range(count))
            ),
            key=lambda p: sum(far[i][p[i]] for i in range(count)),
        )
        for i, d in enumerate(best):
            pairs[i][d] -= 1
        routes.append(best)
    return routes


def route_table(routes):
    count = len(routes[0])
    targets = [list(range(count))] + [list(r) for r in routes]
    sources = [[t.index(i) for i in range(count)] for t in targets]
    return jnp.asarray(np.array([targets, sources], np.int32))


def exchange(slabs, axis, routes):
    return [slabs[0]] + [
        lax.ppermute(slab, axis, list(enumerate(route))) for slab, route in zip(slabs[1:], routes)
    ]


def fast_device(velocity_hat, scalar, tile_offset):
    return fast_step(velocity_hat, scalar, tile_offset)


def fast_step(velocity_hat, scalar, tile_offset):
    length = velocity_hat.shape[4]
    block = velocity_hat.shape[3]
    planes, height, breadth = scalar.shape
    count = lax.axis_size("col")
    rows = lax.axis_size("row")
    wide = 2 * block
    arrival_routes = shift_routes(count)
    wave = np.arange(length)
    wave = np.where(wave < length // 2, wave, wave - length)
    kept = (3 * np.abs(wave) < length).reshape(count, block).any(axis=1)
    departure_routes = needed_routes(count, kept.tolist())
    near = [1 + [r[0] for r in arrival_routes].index(s) for s in (1, count - 1)]
    arrivals, departures = route_table(arrival_routes), route_table(departure_routes)
    y_high, y_low = [jnp.asarray(t) for t in y_table(length)]
    x_high, x_low = [jnp.asarray(t) for t in x_table(length, block)]
    y_specs = [whole_spec(y_high.shape)] * 2
    x_specs = [whole_spec(x_high.shape)] * 2
    edge_rows = 8 * planes * (breadth // wide)
    slab_rows = [
        5 * block + 8 + edge_rows * (s in near) for s in range(count)
    ]
    slabs = kernel_call(
        lambda routes, *refs: inverse_y(count, block, length, routes, near, *refs),
        [arrivals],
        [velocity_hat, scalar, scalar, y_high, y_low],
        [
            whole_spec(velocity_hat.shape),
            pl.BlockSpec((planes, 8, breadth), lambda *_: (0, 0, 0)),
            pl.BlockSpec((planes, 8, breadth), lambda *_: (0, height // 8 - 1, 0)),
        ]
        + y_specs,
        [(r, wide) for r in slab_rows],
        [
            pltpu.VMEM((10 * block, 2 * length), jnp.bfloat16),
            pltpu.VMEM((10 * block, 2 * length), jnp.bfloat16),
            pltpu.VMEM((length, 10 * block), jnp.float32),
        ],
    )
    slabs = exchange(slabs, "col", arrival_routes)
    lines = block + 8
    columns = -(-(breadth // 2 + 3) // wide) * wide
    window_rows = 2 * lines * (columns // wide) + planes * (height + 8)
    results = kernel_call(
        functools.partial(middle, count, rows, block, length, planes, breadth, near),
        [tile_offset, arrivals, departures],
        [*slabs, scalar, scalar, x_high, x_low],
        [whole_spec(s.shape) for s in slabs]
        + [
            pl.BlockSpec((planes, height, wide), lambda *_: (0, 0, 0)),
            pl.BlockSpec((planes, height, wide), lambda *_: (0, 0, breadth // wide - 1)),
        ]
        + x_specs,
        [(3 * block, wide)] * count + [(window_rows, wide)] * rows + [(planes, 8, breadth)],
        [
            pltpu.VMEM((6 * block + 16, 2 * length), jnp.bfloat16),
            pltpu.VMEM((6 * block + 16, 2 * length), jnp.bfloat16),
            pltpu.VMEM((3 * block, 2 * length), jnp.float32),
        ],
    )
    windows = exchange(results[count : count + rows], "row", [
        tuple((i + s) % rows for i in range(rows)) for s in range(1, rows)
    ])
    returned = exchange(results[:count], "col", departure_routes)
    rim = results[count + rows]
    weights = [
        jnp.asarray(row_weights(block, height, block, block + 7)),
        jnp.asarray(row_weights(block, height, block + 2, block + 6)),
        jnp.asarray(column_weights(columns, breadth, breadth + wide)),
    ]
    (scalar_new,) = kernel_call(
        functools.partial(transport, rows, block, planes),
        [],
        [scalar, rim, *windows, *weights],
        [whole_spec(x.shape) for x in (scalar, rim, *windows, *weights)],
        [scalar.shape],
        cost=pl.CostEstimate(flops=4_000_000_000, bytes_accessed=0, transcendentals=0),
    )
    (velocity_new,) = kernel_call(
        functools.partial(forward_y, count, block, length),
        [departures],
        [*returned, velocity_hat, y_high, y_low],
        [whole_spec(x.shape) for x in (*returned, velocity_hat)] + y_specs,
        [velocity_hat.shape],
        [pltpu.VMEM((length, 3 * wide), jnp.float32)],
    )
    return velocity_new, scalar_new


def fits(mesh, velocity_hat, scalar):
    count, rows = mesh.shape["col"], mesh.shape["row"]
    planes = velocity_hat.shape[2] // (mesh.shape["group"] * rows)
    length = velocity_hat.shape[4]
    block = velocity_hat.shape[3] // count
    height, breadth = scalar.shape[1] // count, scalar.shape[2] // rows
    return (
        planes == 1
        and 2 < count <= 8
        and 1 < rows <= 8
        and (2 * block) % 128 == 0
        and height == 2 * block
        and breadth * rows == 2 * length
        and breadth % (2 * block) == 0
        and breadth // 2 + 3 <= length
    )


def solution(mesh):

    def step(velocity_hat, scalar, tile_offset):
        fast = fits(mesh, velocity_hat, scalar)
        mapped = jax.shard_map(
            fast_device if fast else per_device,
            mesh=mesh,
            in_specs=(P(None, None, ("group", "row"), "col", None), P("group", "col", "row"), P()),
            out_specs=(P(None, None, ("group", "row"), "col", None), P("group", "col", "row")),
            check_vma=False,
        )
        return mapped(velocity_hat, scalar, tile_offset)

    return step
```

```python
import functools
import itertools
import math

import jax
import jax.numpy as jnp
import numpy as np
from jax import lax
from jax.experimental import pallas as pl
from jax.experimental.pallas import tpu as pltpu
from jax.sharding import PartitionSpec as P


time_step = 0.25
viscosity = 2.0
diffusivity = 0.15
substep = 0.2
highest = lax.Precision.HIGHEST


def extended(cells, sides, width):
    for axis, dim in sides:
        count = lax.axis_size(axis)
        head = lax.slice_in_dim(cells, 0, width, axis=dim)
        tail = lax.slice_in_dim(cells, cells.shape[dim] - width, cells.shape[dim], axis=dim)
        cells = jnp.concatenate(
            [
                lax.ppermute(tail, axis, [(i, (i + 1) % count) for i in range(count)]),
                cells,
                lax.ppermute(head, axis, [((i + 1) % count, i) for i in range(count)]),
            ],
            axis=dim,
        )
    return cells


def dft_tables(length):
    indices = jnp.arange(length, dtype=jnp.int32)
    phases = indices[:, None] * indices[None, :] % length
    angles = phases.astype(jnp.float32) * (2.0 * math.pi / length)
    factor = 1.0 / math.sqrt(length)
    return (jnp.cos(angles) * factor, jnp.sin(angles) * factor)


def signed_wave(indices, length):
    return jnp.where(indices < length // 2, indices, indices - length)


def transpose_col(packed):
    return lax.all_to_all(packed, "col", split_axis=3, concat_axis=4, tiled=True)


def refine_rows(coarse, margin):
    current = coarse[:, :-1, :]
    following = coarse[:, 1:, :]
    paired = jnp.stack([current, (current + following) * 0.5], axis=2)
    refined = paired.reshape(coarse.shape[0], 2 * (coarse.shape[1] - 1), coarse.shape[2])
    height = 2 * (coarse.shape[1] - 2 * margin)
    return refined[:, margin : margin + height + 2 * margin, :]


def advance(values, x_speed, y_speed):
    height = values.shape[1] - 4
    breadth = values.shape[2] - 4

    def neighbor(step_y, step_x):
        return values[:, 2 + step_y : 2 + step_y + height, 2 + step_x : 2 + step_x + breadth]

    center = neighbor(0, 0)
    grad_x = (neighbor(0, -2) - neighbor(0, 2) + 8.0 * (neighbor(0, 1) - neighbor(0, -1))) / 12.0
    grad_y = (neighbor(-2, 0) - neighbor(2, 0) + 8.0 * (neighbor(1, 0) - neighbor(-1, 0))) / 12.0
    lap_x = (
        16.0 * (neighbor(0, 1) + neighbor(0, -1)) - neighbor(0, 2) - neighbor(0, -2) - 30.0 * center
    ) / 12.0
    lap_y = (
        16.0 * (neighbor(1, 0) + neighbor(-1, 0)) - neighbor(2, 0) - neighbor(-2, 0) - 30.0 * center
    ) / 12.0
    return center + substep * (
        diffusivity * (lap_x + lap_y) - (x_speed * grad_x + y_speed * grad_y)
    )


def per_device(velocity_hat, scalar, tile_offset):
    extent = velocity_hat.shape[4]
    kx_block = velocity_hat.shape[3]
    cosine_table, sine_table = dft_tables(extent)
    wave_all = signed_wave(jnp.arange(extent, dtype=jnp.int32), extent)
    local_wave = signed_wave(
        lax.axis_index("col") * kx_block + jnp.arange(kx_block, dtype=jnp.int32), extent
    )
    kappa_y = (wave_all.astype(jnp.float32) / (extent // 2))[None, None, :]
    kappa_x = (local_wave.astype(jnp.float32) / (extent // 2))[None, :, None]
    real_part = velocity_hat[:, 0]
    imag_part = velocity_hat[:, 1]
    spin_x_real = -kappa_y * imag_part[2]
    spin_x_imag = kappa_y * real_part[2]
    spin_z_real = kappa_y * imag_part[0] - kappa_x * imag_part[1]
    spin_z_imag = kappa_x * real_part[1] - kappa_y * real_part[0]
    fields_real = jnp.concatenate([real_part, jnp.stack([spin_x_real, spin_z_real])])
    fields_imag = jnp.concatenate([imag_part, jnp.stack([spin_x_imag, spin_z_imag])])
    lines_real = jnp.einsum(
        "fpkq,qy->fpyk", fields_real, cosine_table, precision=highest
    ) - jnp.einsum("fpkq,qy->fpyk", fields_imag, sine_table, precision=highest)
    lines_imag = jnp.einsum(
        "fpkq,qy->fpyk", fields_real, sine_table, precision=highest
    ) + jnp.einsum("fpkq,qy->fpyk", fields_imag, cosine_table, precision=highest)
    landed = transpose_col(jnp.stack([lines_real, lines_imag], axis=1))
    landed_real = landed[:, 0]
    landed_imag = landed[:, 1]
    wave_x = (wave_all.astype(jnp.float32) / (extent // 2))[None, None, :]
    spin_y_real = wave_x * landed_imag[2]
    spin_y_imag = -wave_x * landed_real[2]
    landed_real = jnp.concatenate([landed_real[:4], spin_y_real[None], landed_real[4:]])
    landed_imag = jnp.concatenate([landed_imag[:4], spin_y_imag[None], landed_imag[4:]])
    physical = jnp.einsum(
        "fpyk,kx->fpyx", landed_real, cosine_table, precision=highest
    ) - jnp.einsum("fpyk,kx->fpyx", landed_imag, sine_table, precision=highest)
    x_speed = physical[0]
    y_speed = physical[1]
    z_speed = physical[2]
    omega_x = physical[3]
    omega_y = physical[4]
    omega_z = physical[5]
    product = jnp.stack(
        [
            y_speed * omega_z - z_speed * omega_y,
            z_speed * omega_x - x_speed * omega_z,
            x_speed * omega_y - y_speed * omega_x,
        ]
    )
    rows_real = jnp.einsum("cpyx,xk->cpky", product, cosine_table, precision=highest)
    rows_imag = -jnp.einsum("cpyx,xk->cpky", product, sine_table, precision=highest)
    returned = transpose_col(jnp.stack([rows_real, rows_imag], axis=1))
    back_real = returned[:, 0]
    back_imag = returned[:, 1]
    forcing_real = jnp.einsum(
        "cpky,yq->cpkq", back_real, cosine_table, precision=highest
    ) + jnp.einsum("cpky,yq->cpkq", back_imag, sine_table, precision=highest)
    forcing_imag = jnp.einsum(
        "cpky,yq->cpkq", back_imag, cosine_table, precision=highest
    ) - jnp.einsum("cpky,yq->cpkq", back_real, sine_table, precision=highest)
    retained = (3 * jnp.abs(local_wave)[:, None] < extent) & (
        3 * jnp.abs(wave_all)[None, :] < extent
    )
    damping = jnp.exp(-viscosity * time_step * (kappa_x**2 + kappa_y**2))
    new_real = damping * (real_part + time_step * jnp.where(retained, forcing_real, 0.0))
    new_imag = damping * (imag_part + time_step * jnp.where(retained, forcing_imag, 0.0))
    velocity_new = jnp.stack([new_real, new_imag], axis=1)
    horizontal = physical[:2]
    doubled = jnp.concatenate([horizontal, horizontal], axis=3)
    shifted = lax.dynamic_slice_in_dim(doubled, tile_offset[0], extent, 3)
    following = jnp.concatenate([shifted[..., 1:], shifted[..., :1]], axis=3)
    refined_x = jnp.stack([shifted, (shifted + following) * 0.5], axis=4).reshape(
        2, shifted.shape[1], shifted.shape[2], 2 * extent
    )
    arrived = lax.all_to_all(refined_x, "row", split_axis=3, concat_axis=1, tiled=True)
    scalar_ext, x_coarse, y_coarse = (
        extended(scalar, (("row", 2), ("col", 1)), 2),
        extended(arrived[0], (("row", 2), ("col", 1)), 2),
        extended(arrived[1], (("row", 2), ("col", 1)), 2),
    )
    x_refined = refine_rows(x_coarse, 2)[:, 2:-2, 2:-2]
    y_refined = refine_rows(y_coarse, 2)[:, 2:-2, 2:-2]
    halfway = advance(scalar_ext, x_refined, y_refined)
    halfway_ext = extended(halfway, (("row", 2), ("col", 1)), 2)
    scalar_new = advance(halfway_ext, x_refined, y_refined)
    return (velocity_new, scalar_new)


def split(values):
    high = values.astype(jnp.bfloat16)
    return high, (values - high.astype(jnp.float32)).astype(jnp.bfloat16)


def host_split(table):
    table = table.astype(np.float32)
    high = table.astype(jnp.bfloat16)
    return high, (table - high.astype(np.float32)).astype(jnp.bfloat16)


def host_angles(rows, columns, length):
    phases = np.outer(rows, columns) % length
    return phases * (2.0 * np.pi / length)


def y_table(length):
    indices = np.arange(length)
    angles = host_angles(indices, indices, length)
    return host_split(np.concatenate([np.cos(angles), np.sin(angles)], axis=1) / np.sqrt(length))


def x_table(length, block):
    indices = np.arange(length)
    angles = host_angles(indices, indices, length).reshape(length // block, block, length)
    return host_split(
        np.stack([np.cos(angles), -np.sin(angles)], axis=1).reshape(2 * length, length)
        / np.sqrt(length)
    )


def row_weights(lines, height, next_at, last_at):
    weights = np.zeros((height + 8, lines + 8), np.float32)
    place = {**{j: j for j in range(lines)}, lines: next_at, lines + 1: next_at + 1, -1: last_at}
    for fine in range(-2, height + 2):
        base = fine // 2
        row = fine if fine >= 0 else height + 8 + fine
        if fine % 2 == 0:
            weights[row, place[base]] += 1.0
        else:
            weights[row, place[base]] += 0.5
            weights[row, place[base + 1]] += 0.5
    return weights.astype(jnp.bfloat16)


def column_weights(columns, breadth, total):
    weights = np.zeros((columns, total), np.float32)
    for fine in range(-2, breadth + 2):
        base = fine // 2
        at = fine if fine >= 0 else total + fine
        if fine % 2 == 0:
            weights[base + 1, at] += 1.0
        else:
            weights[base + 1, at] += 0.5
            weights[base + 2, at] += 0.5
    return weights.astype(jnp.bfloat16)


def dot(left, right, contract):
    return lax.dot_general(
        left, right, (contract, ((), ())), preferred_element_type=jnp.float32
    )


def dot3(left, right, contract):
    return (
        dot(left[0], right[0], contract)
        + dot(left[0], right[1], contract)
        + dot(left[1], right[0], contract)
    )


def lane_wave(shape, dim, start, length):
    wave = lax.broadcasted_iota(jnp.int32, shape, dim) + start
    return jnp.where(wave < length // 2, wave, wave - length)


def inverse_y(count, block, length, shifts, near, spectra_in, scalar_in, high_in, low_in, *rest):
    outs = rest[:count]
    spectra, head, tail, table_high, table_low, sems = rest[count : count + 6]
    spectra_high, spectra_low, lines = rest[count + 6 :]
    height = scalar_in.shape[1]
    copies = [
        pltpu.make_async_copy(source, target, sems.at[n])
        for n, (source, target) in enumerate(
            (
                (spectra_in, spectra),
                (high_in, table_high),
                (low_in, table_low),
                (scalar_in.at[:, 0:8, :], head),
                (scalar_in.at[:, height - 8 : height, :], tail),
            )
        )
    ]
    for copy in copies:
        copy.start()
    col = lax.axis_index("col")
    copies[0].wait()
    kappa_y = lane_wave((block, length), 1, 0, length).astype(jnp.float32) / (length // 2)
    kappa_x = lane_wave((block, length), 0, col * block, length).astype(jnp.float32) / (length // 2)
    real = [spectra[f, 0, 0] for f in range(3)]
    imag = [spectra[f, 1, 0] for f in range(3)]
    real.append(-kappa_y * imag[2])
    imag.append(kappa_y * real[2])
    real.append(kappa_y * imag[0] - kappa_x * imag[1])
    imag.append(kappa_x * real[1] - kappa_y * real[0])
    for f in range(5):
        real_pair = split(real[f])
        imag_pair = split(imag[f])
        top = slice(2 * f * block, (2 * f + 1) * block)
        bottom = slice((2 * f + 1) * block, (2 * f + 2) * block)
        for store, re, im in (
            (spectra_high, real_pair[0], imag_pair[0]),
            (spectra_low, real_pair[1], imag_pair[1]),
        ):
            store[top, :length] = re
            store[top, length:] = -im
            store[bottom, :length] = im
            store[bottom, length:] = re
    copies[1].wait()
    copies[2].wait()
    lines[...] = dot3(
        (table_high[...], table_low[...]), (spectra_high[...], spectra_low[...]), ((1,), (1,))
    )
    copies[3].wait()
    copies[4].wait()
    wide = 2 * block
    sub = lax.broadcasted_iota(jnp.int32, (8, wide), 0)
    for s in range(count):
        dest = lax.rem(col + shifts[s], count)
        base = pl.multiple_of(dest * block, 8)
        for f in range(5):
            outs[s][f * block : (f + 1) * block, :] = lines[
                pl.ds(base, block), f * wide : (f + 1) * wide
            ]
        following = pl.multiple_of(lax.rem(dest + 1, count) * block, 8)
        before = pl.multiple_of(lax.rem(dest + count - 1, count) * block + block - 8, 8)
        next_x = lines[pl.ds(following, 8), 0:wide]
        next_y = pltpu.roll(lines[pl.ds(following, 8), wide : 2 * wide], 2, 0)
        last_x = lines[pl.ds(before, 8), 0:wide]
        last_y = pltpu.roll(lines[pl.ds(before, 8), wide : 2 * wide], 7, 0)
        rim = jnp.where(sub < 2, next_x, jnp.where(sub < 4, next_y, jnp.where(sub < 7, last_y, last_x)))
        at = 5 * block
        outs[s][at : at + 8, :] = rim
        at += 8
        edges = ([tail] if s == near[0] else []) + ([head] if s == near[1] else [])
        for edge in edges:
            for p in range(edge.shape[0]):
                for b in range(edge.shape[2] // wide):
                    outs[s][at : at + 8, :] = edge[p, :, b * wide : (b + 1) * wide]
                    at += 8


def middle(count, rows, block, length, planes, breadth, near, offsets, arrivals, departures, *refs):
    slabs = refs[:count]
    first, final, table_high, table_low = refs[count : count + 4]
    outs = refs[count + 4 : 2 * count + 4]
    windows = refs[2 * count + 4 : 2 * count + 4 + rows]
    rim_out, lhs_high, lhs_low, freq = refs[2 * count + 4 + rows :]
    col, row, offset = lax.axis_index("col"), lax.axis_index("row"), offsets[0]
    wide = 2 * block
    lane = lax.broadcasted_iota(jnp.int32, (1, wide), 1)
    for s in range(count):
        source = arrivals[1, s, col]
        at = pl.multiple_of(source * wide, wide)
        value = slabs[s][0 : 5 * block, :]
        high, low = split(value)
        lhs_high[0 : 5 * block, pl.ds(at, wide)] = high
        lhs_low[0 : 5 * block, pl.ds(at, wide)] = low
        wave = lax.rem(lane, block) + source * block
        wave = jnp.where(wave < length // 2, wave, wave - length)
        kappa = wave.astype(jnp.float32) / (length // 2)
        kappa = jnp.where(lane < block, kappa, -kappa)
        spin = jnp.concatenate(
            [
                pltpu.roll(value[2 * block : 3 * block], block, 1) * kappa,
                slabs[s][5 * block : 5 * block + 8, :],
                jnp.zeros((8, wide), jnp.float32),
            ]
        )
        high, low = split(spin)
        lhs_high[5 * block :, pl.ds(at, wide)] = high
        lhs_low[5 * block :, pl.ds(at, wide)] = low
    table = (table_high[...], table_low[...])
    physical = dot3((lhs_high[...], lhs_low[...]), table, ((1,), (0,)))
    u, v, w, spin_x, spin_z, spin_y = [physical[f * block : (f + 1) * block] for f in range(6)]
    product = jnp.concatenate([v * spin_z - w * spin_y, w * spin_x - u * spin_z, u * spin_y - v * spin_x])
    freq[...] = dot3(split(product), table, ((1,), (1,)))
    for s in range(count):
        at = pl.multiple_of(departures[0, s, col] * wide, wide)
        outs[s][...] = freq[:, pl.ds(at, wide)]
    rim = physical[6 * block : 6 * block + 8]
    sub = lax.broadcasted_iota(jnp.int32, (8, wide), 0)
    pieces = breadth // wide
    edge = 5 * block + 8
    for p in range(planes):
        for b in range(pieces):
            step = 8 * (p * pieces + b)
            upper = slabs[near[0]][edge + step : edge + step + 8, :]
            lower = slabs[near[1]][edge + step : edge + step + 8, :]
            rim_out[p, :, b * wide : (b + 1) * wide] = jnp.where(sub < 4, lower, upper)
    cells = breadth // 2
    height = first.shape[1]
    kept = windows[0].shape[0] - planes * (height + 8)
    lines = block + 8
    span = kept // (2 * lines)
    for s in range(rows):
        target = lax.rem(row + s, rows)
        shift = lax.rem(2 * length + 1 - offset - target * cells, length)
        for f, field in enumerate((u, v)):
            rolled = pltpu.roll(jnp.concatenate([field, rim]), shift, 1)
            for b in range(span):
                at = (f * span + b) * lines
                windows[s][at : at + lines, :] = rolled[:, b * wide : (b + 1) * wide]
        if s > 0:
            for p in range(planes):
                at = kept + p * (height + 8)
                windows[s][at : at + height, :] = jnp.where(lane < block, first[p], final[p])
                windows[s][at + height : at + height + 8, :] = jnp.where(
                    lane < block, rim_out[p, :, 0:wide], rim_out[p, :, breadth - wide : breadth]
                )


def transport(rows, block, planes, *refs):
    scalar, rim = refs[0], refs[1]
    windows = refs[2 : 2 + rows]
    weights_x, weights_y, across, out = refs[2 + rows :]
    row = lax.axis_index("row")
    wide = 2 * block
    height, breadth = scalar.shape[1], scalar.shape[2]
    lines = block + 8
    kept = windows[0].shape[0] - planes * (height + 8)
    span = kept // (2 * lines)
    lane = lax.broadcasted_iota(jnp.int32, (1, wide), 1)
    per_row = planes // rows
    tall = height + 8

    def shifted(values, amount, axis):
        return pltpu.roll(values, (-amount) % values.shape[axis], axis)

    for s in range(rows):
        source = lax.rem(row + rows - s, rows)
        speeds = []
        for f, weights in enumerate((weights_x, weights_y)):
            coarse = jnp.concatenate(
                [windows[s][(f * span + b) * lines : (f * span + b + 1) * lines, :] for b in range(span)],
                axis=1,
            )
            high, low = split(coarse)
            taller = dot(weights[...], high, ((1,), (0,))) + dot(weights[...], low, ((1,), (0,)))
            high, low = split(taller)
            speeds.append(dot(high, across[...], ((1,), (0,))) + dot(low, across[...], ((1,), (0,))))
        x_speed, y_speed = speeds
        for q in range(per_row):
            p = source * per_row + q
            sides = []
            for part in (1 % rows, rows - 1):
                sides.append(windows[part][pl.ds(pl.multiple_of(kept + p * tall, 8), tall), :])
            values = jnp.concatenate(
                [
                    jnp.concatenate([scalar[p], rim[p]], axis=0),
                    jnp.where(lane < block, sides[1], sides[0]),
                ],
                axis=1,
            )
            for _ in range(2):
                right, left = shifted(values, 1, 1), shifted(values, -1, 1)
                right2, left2 = shifted(values, 2, 1), shifted(values, -2, 1)
                below, above = shifted(values, 1, 0), shifted(values, -1, 0)
                below2, above2 = shifted(values, 2, 0), shifted(values, -2, 0)
                grad_x = left2 - right2 + 8.0 * (right - left)
                grad_y = above2 - below2 + 8.0 * (below - above)
                near = (right + left) + (below + above)
                far = (right2 + left2) + (below2 + above2)
                spread = 16.0 * near - far - 60.0 * values
                values = values + (substep / 12.0) * (
                    diffusivity * spread - (x_speed * grad_x + y_speed * grad_y)
                )
            out[p] = values[:height, :breadth]


def forward_y(count, block, length, departures, *refs):
    slabs = refs[:count]
    spectra, table_high, table_low, out, gathered = refs[count:]
    col = lax.axis_index("col")
    wide = 2 * block
    for s in range(count):
        source = departures[1, s, col]
        at = pl.multiple_of(source * block, 8)
        for f in range(3):
            gathered[pl.ds(at, block), f * wide : (f + 1) * wide] = slabs[s][
                f * block : (f + 1) * block, :
            ]
    parts = dot3(split(gathered[...].T), (table_high[...], table_low[...]), ((1,), (0,)))
    wave_y = lane_wave((block, length), 1, 0, length)
    wave_x = lane_wave((block, length), 0, col * block, length)
    kappa_y = wave_y.astype(jnp.float32) / (length // 2)
    kappa_x = wave_x.astype(jnp.float32) / (length // 2)
    damping = jnp.exp(-viscosity * time_step * (kappa_x * kappa_x + kappa_y * kappa_y))
    retained = (3 * jnp.abs(wave_x) < length) & (3 * jnp.abs(wave_y) < length)
    for f in range(3):
        real = parts[f * wide : f * wide + block]
        imag = parts[f * wide + block : (f + 1) * wide]
        forcing_real = real[:, :length] + imag[:, length:]
        forcing_imag = imag[:, :length] - real[:, length:]
        out[f, 0, 0] = damping * (
            spectra[f, 0, 0] + time_step * jnp.where(retained, forcing_real, 0.0)
        )
        out[f, 1, 0] = damping * (
            spectra[f, 1, 0] + time_step * jnp.where(retained, forcing_imag, 0.0)
        )


def whole_spec(shape):
    return pl.BlockSpec(shape, lambda *_: (0,) * len(shape))


def kernel_call(body, scalars, operands, specs, out_shapes, scratch=(), cost=None):
    return pl.pallas_call(
        body,
        grid=(1,),
        in_specs=[pl.BlockSpec(memory_space=pltpu.SMEM)] * len(scalars) + specs,
        out_specs=[whole_spec(s) for s in out_shapes],
        out_shape=[jax.ShapeDtypeStruct(s, jnp.float32) for s in out_shapes],
        scratch_shapes=list(scratch),
        compiler_params=pltpu.CompilerParams(vmem_limit_bytes=20 * 1024 * 1024),
        cost_estimate=cost,
    )(*scalars, *operands)


def shift_routes(count):
    order = sorted(range(1, count), key=lambda s: (-min(s, count - s), s))
    return [tuple((i + s) % count for i in range(count)) for s in order]


def needed_routes(count, needed):
    pairs = [[int(needed[d] and i != d) for d in range(count)] for i in range(count)]
    spare = [i for i in range(count) for _ in range(count - 1 - sum(pairs[i]))]
    idle = [d for d in range(count) if not needed[d] for _ in range(count - 1)]
    for i, d in zip(spare, idle):
        pairs[i][d] += 1
    far = [[2 * abs(i - d) if needed[d] else 0 for d in range(count)] for i in range(count)]
    routes = []
    for _ in range(count - 1):
        best = max(
            (
                p
                for p in itertools.permutations(range(count))
                if all(pairs[i][p[i]] for i in range(count))
            ),
            key=lambda p: sum(far[i][p[i]] for i in range(count)),
        )
        for i, d in enumerate(best):
            pairs[i][d] -= 1
        routes.append(best)
    return routes


def route_table(routes):
    count = len(routes[0])
    targets = [list(range(count))] + [list(r) for r in routes]
    sources = [[t.index(i) for i in range(count)] for t in targets]
    return jnp.asarray(np.array([targets, sources], np.int32))


def exchange(slabs, axis, routes):
    arrived = [slabs[0]]
    for slab, route in zip(slabs[1:], routes):
        arrived.append(lax.ppermute(slab, axis, list(enumerate(route))))
    return arrived


def fast_device(velocity_hat, scalar, tile_offset):
    return fast_step(velocity_hat, scalar, tile_offset)


def fast_step(velocity_hat, scalar, tile_offset):
    length = velocity_hat.shape[4]
    block = velocity_hat.shape[3]
    planes, height, breadth = scalar.shape
    count = lax.axis_size("col")
    rows = lax.axis_size("row")
    wide = 2 * block
    arrival_routes = shift_routes(count)
    wave = np.arange(length)
    wave = np.where(wave < length // 2, wave, wave - length)
    kept = (3 * np.abs(wave) < length).reshape(count, block).any(axis=1)
    departure_routes = needed_routes(count, kept.tolist())
    near = [1 + [r[0] for r in arrival_routes].index(s) for s in (1, count - 1)]
    arrivals, departures = route_table(arrival_routes), route_table(departure_routes)
    y_high, y_low = [jnp.asarray(t) for t in y_table(length)]
    x_high, x_low = [jnp.asarray(t) for t in x_table(length, block)]
    y_specs = [whole_spec(y_high.shape)] * 2
    x_specs = [whole_spec(x_high.shape)] * 2
    edge_rows = 8 * planes * (breadth // wide)
    slab_rows = [
        5 * block + 8 + edge_rows * (s in near) for s in range(count)
    ]
    hbm = pl.BlockSpec(memory_space=pltpu.HBM)
    slabs = kernel_call(
        functools.partial(inverse_y, count, block, length, [0] + [r[0] for r in arrival_routes], near),
        [],
        [
            pltpu.with_memory_space_constraint(x, pltpu.HBM)
            for x in (velocity_hat, scalar, y_high, y_low)
        ],
        [hbm] * 4,
        [(r, wide) for r in slab_rows],
        [
            pltpu.VMEM(velocity_hat.shape, jnp.float32),
            pltpu.VMEM((planes, 8, breadth), jnp.float32),
            pltpu.VMEM((planes, 8, breadth), jnp.float32),
            pltpu.VMEM(y_high.shape, jnp.bfloat16),
            pltpu.VMEM(y_low.shape, jnp.bfloat16),
            pltpu.SemaphoreType.DMA((5,)),
            pltpu.VMEM((10 * block, 2 * length), jnp.bfloat16),
            pltpu.VMEM((10 * block, 2 * length), jnp.bfloat16),
            pltpu.VMEM((length, 10 * block), jnp.float32),
        ],
    )
    slabs = exchange(slabs, "col", arrival_routes)
    lines = block + 8
    columns = -(-(breadth // 2 + 3) // wide) * wide
    window_rows = 2 * lines * (columns // wide) + planes * (height + 8)
    results = kernel_call(
        functools.partial(middle, count, rows, block, length, planes, breadth, near),
        [tile_offset, arrivals, departures],
        [*slabs, scalar, scalar, x_high, x_low],
        [whole_spec(s.shape) for s in slabs]
        + [
            pl.BlockSpec((planes, height, wide), lambda *_: (0, 0, 0)),
            pl.BlockSpec((planes, height, wide), lambda *_: (0, 0, breadth // wide - 1)),
        ]
        + x_specs,
        [(3 * block, wide)] * count + [(window_rows, wide)] * rows + [(planes, 8, breadth)],
        [
            pltpu.VMEM((6 * block + 16, 2 * length), jnp.bfloat16),
            pltpu.VMEM((6 * block + 16, 2 * length), jnp.bfloat16),
            pltpu.VMEM((3 * block, 2 * length), jnp.float32),
        ],
    )
    windows = exchange(results[count : count + rows], "row", [
        tuple((i + s) % rows for i in range(rows)) for s in range(1, rows)
    ])
    returned = exchange(results[:count], "col", departure_routes)
    rim = results[count + rows]
    weights = [
        jnp.asarray(row_weights(block, height, block, block + 7)),
        jnp.asarray(row_weights(block, height, block + 2, block + 6)),
        jnp.asarray(column_weights(columns, breadth, breadth + wide)),
    ]
    (scalar_new,) = kernel_call(
        functools.partial(transport, rows, block, planes),
        [],
        [scalar, rim, *windows, *weights],
        [whole_spec(x.shape) for x in (scalar, rim, *windows, *weights)],
        [scalar.shape],
        cost=pl.CostEstimate(flops=4_000_000_000, bytes_accessed=0, transcendentals=0),
    )
    (velocity_new,) = kernel_call(
        functools.partial(forward_y, count, block, length),
        [departures],
        [*returned, velocity_hat, y_high, y_low],
        [whole_spec(x.shape) for x in (*returned, velocity_hat)] + y_specs,
        [velocity_hat.shape],
        [pltpu.VMEM((length, 3 * wide), jnp.float32)],
    )
    return velocity_new, scalar_new


def fits(mesh, velocity_hat, scalar):
    count, rows = mesh.shape["col"], mesh.shape["row"]
    planes = velocity_hat.shape[2] // (mesh.shape["group"] * rows)
    length = velocity_hat.shape[4]
    block = velocity_hat.shape[3] // count
    height, breadth = scalar.shape[1] // count, scalar.shape[2] // rows
    return (
        planes == 1
        and 2 < count <= 8
        and 1 < rows <= 8
        and (2 * block) % 128 == 0
        and height == 2 * block
        and breadth * rows == 2 * length
        and breadth % (2 * block) == 0
        and breadth // 2 + 3 <= length
    )


def solution(mesh):
    def step(velocity_hat, scalar, tile_offset):
        fast = fits(mesh, velocity_hat, scalar)
        mapped = jax.shard_map(
            fast_device if fast else per_device,
            mesh=mesh,
            in_specs=(P(None, None, ("group", "row"), "col", None), P("group", "col", "row"), P()),
            out_specs=(P(None, None, ("group", "row"), "col", None), P("group", "col", "row")),
            check_vma=False,
        )
        return mapped(velocity_hat, scalar, tile_offset)

    return step
```

```python
import functools
import itertools
import math

import jax
import jax.numpy as jnp
import numpy as np
from jax import lax
from jax.experimental import pallas as pl
from jax.experimental.pallas import tpu as pltpu
from jax.sharding import PartitionSpec as P


time_step = 0.25
viscosity = 2.0
diffusivity = 0.15
substep = 0.2
highest = lax.Precision.HIGHEST


def extended(cells, sides, width):
    for axis, dim in sides:
        count = lax.axis_size(axis)
        head = lax.slice_in_dim(cells, 0, width, axis=dim)
        tail = lax.slice_in_dim(cells, cells.shape[dim] - width, cells.shape[dim], axis=dim)
        cells = jnp.concatenate(
            [
                lax.ppermute(tail, axis, [(i, (i + 1) % count) for i in range(count)]),
                cells,
                lax.ppermute(head, axis, [((i + 1) % count, i) for i in range(count)]),
            ],
            axis=dim,
        )
    return cells


def dft_tables(length):
    indices = jnp.arange(length, dtype=jnp.int32)
    phases = indices[:, None] * indices[None, :] % length
    angles = phases.astype(jnp.float32) * (2.0 * math.pi / length)
    factor = 1.0 / math.sqrt(length)
    return (jnp.cos(angles) * factor, jnp.sin(angles) * factor)


def signed_wave(indices, length):
    return jnp.where(indices < length // 2, indices, indices - length)


def transpose_col(packed):
    return lax.all_to_all(packed, "col", split_axis=3, concat_axis=4, tiled=True)


def refine_rows(coarse, margin):
    current = coarse[:, :-1, :]
    following = coarse[:, 1:, :]
    paired = jnp.stack([current, (current + following) * 0.5], axis=2)
    refined = paired.reshape(coarse.shape[0], 2 * (coarse.shape[1] - 1), coarse.shape[2])
    height = 2 * (coarse.shape[1] - 2 * margin)
    return refined[:, margin : margin + height + 2 * margin, :]


def advance(values, x_speed, y_speed):
    height = values.shape[1] - 4
    breadth = values.shape[2] - 4

    def neighbor(step_y, step_x):
        return values[:, 2 + step_y : 2 + step_y + height, 2 + step_x : 2 + step_x + breadth]

    center = neighbor(0, 0)
    grad_x = (neighbor(0, -2) - neighbor(0, 2) + 8.0 * (neighbor(0, 1) - neighbor(0, -1))) / 12.0
    grad_y = (neighbor(-2, 0) - neighbor(2, 0) + 8.0 * (neighbor(1, 0) - neighbor(-1, 0))) / 12.0
    lap_x = (
        16.0 * (neighbor(0, 1) + neighbor(0, -1)) - neighbor(0, 2) - neighbor(0, -2) - 30.0 * center
    ) / 12.0
    lap_y = (
        16.0 * (neighbor(1, 0) + neighbor(-1, 0)) - neighbor(2, 0) - neighbor(-2, 0) - 30.0 * center
    ) / 12.0
    return center + substep * (
        diffusivity * (lap_x + lap_y) - (x_speed * grad_x + y_speed * grad_y)
    )


def per_device(velocity_hat, scalar, tile_offset):
    extent = velocity_hat.shape[4]
    kx_block = velocity_hat.shape[3]
    cosine_table, sine_table = dft_tables(extent)
    wave_all = signed_wave(jnp.arange(extent, dtype=jnp.int32), extent)
    local_wave = signed_wave(
        lax.axis_index("col") * kx_block + jnp.arange(kx_block, dtype=jnp.int32), extent
    )
    kappa_y = (wave_all.astype(jnp.float32) / (extent // 2))[None, None, :]
    kappa_x = (local_wave.astype(jnp.float32) / (extent // 2))[None, :, None]
    real_part = velocity_hat[:, 0]
    imag_part = velocity_hat[:, 1]
    spin_x_real = -kappa_y * imag_part[2]
    spin_x_imag = kappa_y * real_part[2]
    spin_z_real = kappa_y * imag_part[0] - kappa_x * imag_part[1]
    spin_z_imag = kappa_x * real_part[1] - kappa_y * real_part[0]
    fields_real = jnp.concatenate([real_part, jnp.stack([spin_x_real, spin_z_real])])
    fields_imag = jnp.concatenate([imag_part, jnp.stack([spin_x_imag, spin_z_imag])])
    lines_real = jnp.einsum(
        "fpkq,qy->fpyk", fields_real, cosine_table, precision=highest
    ) - jnp.einsum("fpkq,qy->fpyk", fields_imag, sine_table, precision=highest)
    lines_imag = jnp.einsum(
        "fpkq,qy->fpyk", fields_real, sine_table, precision=highest
    ) + jnp.einsum("fpkq,qy->fpyk", fields_imag, cosine_table, precision=highest)
    landed = transpose_col(jnp.stack([lines_real, lines_imag], axis=1))
    landed_real = landed[:, 0]
    landed_imag = landed[:, 1]
    wave_x = (wave_all.astype(jnp.float32) / (extent // 2))[None, None, :]
    spin_y_real = wave_x * landed_imag[2]
    spin_y_imag = -wave_x * landed_real[2]
    landed_real = jnp.concatenate([landed_real[:4], spin_y_real[None], landed_real[4:]])
    landed_imag = jnp.concatenate([landed_imag[:4], spin_y_imag[None], landed_imag[4:]])
    physical = jnp.einsum(
        "fpyk,kx->fpyx", landed_real, cosine_table, precision=highest
    ) - jnp.einsum("fpyk,kx->fpyx", landed_imag, sine_table, precision=highest)
    x_speed = physical[0]
    y_speed = physical[1]
    z_speed = physical[2]
    omega_x = physical[3]
    omega_y = physical[4]
    omega_z = physical[5]
    product = jnp.stack(
        [
            y_speed * omega_z - z_speed * omega_y,
            z_speed * omega_x - x_speed * omega_z,
            x_speed * omega_y - y_speed * omega_x,
        ]
    )
    rows_real = jnp.einsum("cpyx,xk->cpky", product, cosine_table, precision=highest)
    rows_imag = -jnp.einsum("cpyx,xk->cpky", product, sine_table, precision=highest)
    returned = transpose_col(jnp.stack([rows_real, rows_imag], axis=1))
    back_real = returned[:, 0]
    back_imag = returned[:, 1]
    forcing_real = jnp.einsum(
        "cpky,yq->cpkq", back_real, cosine_table, precision=highest
    ) + jnp.einsum("cpky,yq->cpkq", back_imag, sine_table, precision=highest)
    forcing_imag = jnp.einsum(
        "cpky,yq->cpkq", back_imag, cosine_table, precision=highest
    ) - jnp.einsum("cpky,yq->cpkq", back_real, sine_table, precision=highest)
    retained = (3 * jnp.abs(local_wave)[:, None] < extent) & (
        3 * jnp.abs(wave_all)[None, :] < extent
    )
    damping = jnp.exp(-viscosity * time_step * (kappa_x**2 + kappa_y**2))
    new_real = damping * (real_part + time_step * jnp.where(retained, forcing_real, 0.0))
    new_imag = damping * (imag_part + time_step * jnp.where(retained, forcing_imag, 0.0))
    velocity_new = jnp.stack([new_real, new_imag], axis=1)
    horizontal = physical[:2]
    doubled = jnp.concatenate([horizontal, horizontal], axis=3)
    shifted = lax.dynamic_slice_in_dim(doubled, tile_offset[0], extent, 3)
    following = jnp.concatenate([shifted[..., 1:], shifted[..., :1]], axis=3)
    refined_x = jnp.stack([shifted, (shifted + following) * 0.5], axis=4).reshape(
        2, shifted.shape[1], shifted.shape[2], 2 * extent
    )
    arrived = lax.all_to_all(refined_x, "row", split_axis=3, concat_axis=1, tiled=True)
    scalar_ext, x_coarse, y_coarse = (
        extended(scalar, (("row", 2), ("col", 1)), 2),
        extended(arrived[0], (("row", 2), ("col", 1)), 2),
        extended(arrived[1], (("row", 2), ("col", 1)), 2),
    )
    x_refined = refine_rows(x_coarse, 2)[:, 2:-2, 2:-2]
    y_refined = refine_rows(y_coarse, 2)[:, 2:-2, 2:-2]
    halfway = advance(scalar_ext, x_refined, y_refined)
    halfway_ext = extended(halfway, (("row", 2), ("col", 1)), 2)
    scalar_new = advance(halfway_ext, x_refined, y_refined)
    return (velocity_new, scalar_new)


def split(values):
    high = values.astype(jnp.bfloat16)
    return high, (values - high.astype(jnp.float32)).astype(jnp.bfloat16)


def host_split(table):
    table = table.astype(np.float32)
    high = table.astype(jnp.bfloat16)
    return high, (table - high.astype(np.float32)).astype(jnp.bfloat16)


def host_angles(rows, columns, length):
    phases = np.outer(rows, columns) % length
    return phases * (2.0 * np.pi / length)


margin = 16


def y_table(length):
    rows = np.arange(-margin, length + margin) % length
    angles = host_angles(rows, np.arange(length), length)
    return host_split(np.concatenate([np.cos(angles), np.sin(angles)], axis=1) / np.sqrt(length))


def row_weights(lines, height, next_at, last_at):
    weights = np.zeros((height + 8, lines + 8), np.float32)
    place = {**{j: j for j in range(lines)}, lines: next_at, lines + 1: next_at + 1, -1: last_at}
    for fine in range(-2, height + 2):
        base = fine // 2
        row = fine if fine >= 0 else height + 8 + fine
        if fine % 2 == 0:
            weights[row, place[base]] += 1.0
        else:
            weights[row, place[base]] += 0.5
            weights[row, place[base + 1]] += 0.5
    return weights.astype(jnp.bfloat16)


def column_weights(columns, breadth, total):
    base = lax.broadcasted_iota(jnp.int32, (columns, total), 0) - 1
    fine = lax.broadcasted_iota(jnp.int32, (columns, total), 1)
    fine = jnp.where(fine < breadth + 2, fine, fine - total)
    twice = jnp.abs(2 * base - fine)
    at_point = jnp.where(fine % 2 == 0, jnp.where(twice == 0, 1.0, 0.0), jnp.where(twice == 1, 0.5, 0.0))
    return jnp.where(fine >= -2, at_point, 0.0).astype(jnp.bfloat16)


def dot(left, right, contract):
    return lax.dot_general(
        left, right, (contract, ((), ())), preferred_element_type=jnp.float32
    )


def dot3(left, right, contract):
    return (
        dot(left[0], right[0], contract)
        + dot(left[0], right[1], contract)
        + dot(left[1], right[0], contract)
    )


def lane_wave(shape, dim, start, length):
    wave = lax.broadcasted_iota(jnp.int32, shape, dim) + start
    return jnp.where(wave < length // 2, wave, wave - length)


def inverse_y(count, block, length, deltas, spectra_in, scalar_in, high_in, low_in, *rest):
    outs, edges = rest[: len(deltas)], rest[len(deltas) : -7]
    spectra, table_high, table_low, sems, spectra_high, spectra_low, lines = rest[-7:]
    height = scalar_in.shape[1]
    col = lax.axis_index("col")
    half = count // 2
    reach = half * block
    side = lax.div(lax.bitwise_xor(col, deltas[0]), half)
    rows = pl.ds(pl.multiple_of(side * reach, 16), reach + 2 * margin)
    pieces = [
        (spectra_in, spectra),
        (high_in.at[rows, :], table_high),
        (low_in.at[rows, :], table_low),
    ]
    if edges:
        pieces += [
            (scalar_in.at[:, height - 8 : height, :], edges[0]),
            (scalar_in.at[:, 0:8, :], edges[1]),
        ]
    copies = [
        pltpu.make_async_copy(source, target, sems.at[n])
        for n, (source, target) in enumerate(pieces)
    ]
    for copy in copies:
        copy.start()
    copies[0].wait()
    kappa_y = lane_wave((block, length), 1, 0, length).astype(jnp.float32) / (length // 2)
    kappa_x = lane_wave((block, length), 0, col * block, length).astype(jnp.float32) / (length // 2)
    real = [spectra[f, 0, 0] for f in range(3)]
    imag = [spectra[f, 1, 0] for f in range(3)]
    real.append(-kappa_y * imag[2])
    imag.append(kappa_y * real[2])
    real.append(kappa_y * imag[0] - kappa_x * imag[1])
    imag.append(kappa_x * real[1] - kappa_y * real[0])
    for f in range(5):
        real_pair = split(real[f])
        imag_pair = split(imag[f])
        top = slice(2 * f * block, (2 * f + 1) * block)
        bottom = slice((2 * f + 1) * block, (2 * f + 2) * block)
        for store, re, im in (
            (spectra_high, real_pair[0], imag_pair[0]),
            (spectra_low, real_pair[1], imag_pair[1]),
        ):
            store[top, :length] = re
            store[top, length:] = -im
            store[bottom, :length] = im
            store[bottom, length:] = re
    for copy in copies[1:]:
        copy.wait()
    lines[...] = dot3(
        (table_high[...], table_low[...]), (spectra_high[...], spectra_low[...]), ((1,), (1,))
    )
    wide = 2 * block
    sub = lax.broadcasted_iota(jnp.int32, (8, wide), 0)
    for delta, out in zip(deltas, outs):
        dest = lax.bitwise_and(lax.bitwise_xor(col, delta), half - 1)
        base = pl.multiple_of(margin + dest * block, 8)
        for f in range(5):
            out[f * block : (f + 1) * block, :] = lines[
                pl.ds(base, block), f * wide : (f + 1) * wide
            ]
        following, before = pl.ds(base + block, 8), pl.ds(base - 8, 8)
        next_x = lines[following, 0:wide]
        next_y = pltpu.roll(lines[following, wide : 2 * wide], 2, 0)
        last_x = lines[before, 0:wide]
        last_y = pltpu.roll(lines[before, wide : 2 * wide], 7, 0)
        rim = jnp.where(sub < 2, next_x, jnp.where(sub < 4, next_y, jnp.where(sub < 7, last_y, last_x)))
        out[5 * block : 5 * block + 8, :] = rim


def place_slabs(count, block, length, deltas, slabs, lhs_high, lhs_low):
    col = lax.axis_index("col")
    wide = 2 * block
    lane = lax.broadcasted_iota(jnp.int32, (1, wide), 1)
    for delta, slab in zip(deltas, slabs):
        source = lax.bitwise_xor(col, delta)
        at = pl.ds(pl.multiple_of(lax.bitwise_and(source, count // 2 - 1) * wide, wide), wide)
        value = slab[0 : 5 * block, :]
        high, low = split(value)
        lhs_high[0 : 5 * block, at] = high
        lhs_low[0 : 5 * block, at] = low
        wave = lax.rem(lane, block) + source * block
        wave = jnp.where(wave < length // 2, wave, wave - length)
        kappa = wave.astype(jnp.float32) / (length // 2)
        kappa = jnp.where(lane < block, kappa, -kappa)
        spin = jnp.concatenate(
            [
                pltpu.roll(value[2 * block : 3 * block], block, 1) * kappa,
                slab[5 * block : 5 * block + 8, :],
                jnp.zeros((8, wide), jnp.float32),
            ]
        )
        high, low = split(spin)
        lhs_high[5 * block :, at] = high
        lhs_low[5 * block :, at] = low


def partial_x(count, block, length, deltas, *refs):
    slabs = refs[: len(deltas)]
    y_high, y_low, out, table_high, table_low, lhs_high, lhs_low = refs[len(deltas) :]
    col = lax.axis_index("col")
    for source, target in ((y_high, table_high), (y_low, table_low)):
        for c in range(count):
            rows = slice(margin + c * block, margin + (c + 1) * block)
            target[2 * c * block : (2 * c + 1) * block, :] = source[rows, 0:length]
            target[(2 * c + 1) * block : (2 * c + 2) * block, :] = -source[rows, length:]
    place_slabs(count, block, length, deltas, slabs, lhs_high, lhs_low)
    side = lax.div(lax.bitwise_xor(col, deltas[0]), count // 2)
    rows = pl.ds(pl.multiple_of(side * length, 16), length)
    out[...] = dot3(
        (lhs_high[...], lhs_low[...]), (table_high[rows, :], table_low[rows, :]), ((1,), (0,))
    )


def middle(count, rows, block, length, planes, breadth, deltas, offsets, departures, *refs):
    slabs = refs[: len(deltas)]
    near_sum, upper_edge, lower_edge, first, final, table_high, table_low = refs[
        len(deltas) : len(deltas) + 7
    ]
    refs = refs[len(deltas) + 7 :]
    outs, windows = refs[:count], refs[count : count + rows]
    rim_out, lhs_high, lhs_low, freq = refs[count + rows :]
    col, row, offset = lax.axis_index("col"), lax.axis_index("row"), offsets[0]
    wide = 2 * block
    lane = lax.broadcasted_iota(jnp.int32, (1, wide), 1)
    place_slabs(count, block, length, deltas, slabs, lhs_high, lhs_low)
    side = lax.div(lax.bitwise_xor(col, deltas[0]), count // 2)
    half_rows = pl.ds(pl.multiple_of(side * length, 16), length)
    physical = near_sum[...] + dot3(
        (lhs_high[...], lhs_low[...]),
        (table_high[half_rows, :], table_low[half_rows, :]),
        ((1,), (0,)),
    )
    table = (table_high[...], table_low[...])
    u, v, w, spin_x, spin_z, spin_y = [physical[f * block : (f + 1) * block] for f in range(6)]
    product = jnp.concatenate([v * spin_z - w * spin_y, w * spin_x - u * spin_z, u * spin_y - v * spin_x])
    freq[...] = dot3(split(product), table, ((1,), (1,)))
    for s in range(count):
        at = pl.multiple_of(departures[0, s, col] * wide, wide)
        outs[s][...] = freq[:, pl.ds(at, wide)]
    rim = physical[6 * block : 6 * block + 8]
    edge_sub = lax.broadcasted_iota(jnp.int32, (8, breadth), 0)
    for p in range(planes):
        rim_out[p] = jnp.where(edge_sub < 4, lower_edge[p], upper_edge[p])
    cells = breadth // 2
    height = first.shape[1]
    kept = windows[0].shape[0] - planes * (height + 8)
    lines = block + 8
    span = kept // (2 * lines)
    for s in range(rows):
        target = lax.rem(row + s, rows)
        shift = lax.rem(2 * length + 1 - offset - target * cells, length)
        for f, field in enumerate((u, v)):
            rolled = pltpu.roll(jnp.concatenate([field, rim]), shift, 1)
            for b in range(span):
                at = (f * span + b) * lines
                windows[s][at : at + lines, :] = rolled[:, b * wide : (b + 1) * wide]
        if s > 0:
            for p in range(planes):
                at = kept + p * (height + 8)
                windows[s][at : at + height, :] = jnp.where(lane < block, first[p], final[p])
                windows[s][at + height : at + height + 8, :] = jnp.where(
                    lane < block, rim_out[p, :, 0:wide], rim_out[p, :, breadth - wide : breadth]
                )


def transport(rows, block, planes, *refs):
    scalar, rim = refs[0], refs[1]
    windows = refs[2 : 2 + rows]
    weights_x, weights_y, out = refs[2 + rows :]
    row = lax.axis_index("row")
    wide = 2 * block
    height, breadth = scalar.shape[1], scalar.shape[2]
    lines = block + 8
    kept = windows[0].shape[0] - planes * (height + 8)
    span = kept // (2 * lines)
    lane = lax.broadcasted_iota(jnp.int32, (1, wide), 1)
    per_row = planes // rows
    tall, total = height + 8, breadth + wide
    across = column_weights(span * wide, breadth, total)

    def shifted(values, amount, axis):
        return pltpu.roll(values, (-amount) % values.shape[axis], axis)

    for s in range(rows):
        source = lax.rem(row + rows - s, rows)
        speeds = []
        for f, weights in enumerate((weights_x, weights_y)):
            coarse = jnp.concatenate(
                [windows[s][(f * span + b) * lines : (f * span + b + 1) * lines, :] for b in range(span)],
                axis=1,
            )
            high, low = split(coarse)
            taller = dot(weights[...], high, ((1,), (0,))) + dot(weights[...], low, ((1,), (0,)))
            high, low = split(taller)
            speeds.append(dot(high, across, ((1,), (0,))) + dot(low, across, ((1,), (0,))))
        x_speed, y_speed = speeds
        for q in range(per_row):
            p = source * per_row + q
            sides = []
            for part in (1 % rows, rows - 1):
                sides.append(windows[part][pl.ds(pl.multiple_of(kept + p * tall, 8), tall), :])
            values = jnp.concatenate(
                [
                    jnp.concatenate([scalar[p], rim[p]], axis=0),
                    jnp.where(lane < block, sides[1], sides[0]),
                ],
                axis=1,
            )
            for _ in range(2):
                right, left = shifted(values, 1, 1), shifted(values, -1, 1)
                right2, left2 = shifted(values, 2, 1), shifted(values, -2, 1)
                below, above = shifted(values, 1, 0), shifted(values, -1, 0)
                below2, above2 = shifted(values, 2, 0), shifted(values, -2, 0)
                grad_x = left2 - right2 + 8.0 * (right - left)
                grad_y = above2 - below2 + 8.0 * (below - above)
                near = (right + left) + (below + above)
                far = (right2 + left2) + (below2 + above2)
                spread = 16.0 * near - far - 60.0 * values
                values = values + (substep / 12.0) * (
                    diffusivity * spread - (x_speed * grad_x + y_speed * grad_y)
                )
            out[p] = values[:height, :breadth]


def forward_y(count, block, length, departures, *refs):
    slabs = refs[:count]
    spectra, table_high, table_low, out, gathered = refs[count:]
    col = lax.axis_index("col")
    wide = 2 * block
    for s in range(count):
        source = departures[1, s, col]
        at = pl.multiple_of(source * block, 8)
        for f in range(3):
            gathered[pl.ds(at, block), f * wide : (f + 1) * wide] = slabs[s][
                f * block : (f + 1) * block, :
            ]
    inner = slice(margin, margin + length)
    parts = dot3(
        split(gathered[...].T), (table_high[inner, :], table_low[inner, :]), ((1,), (0,))
    )
    wave_y = lane_wave((block, length), 1, 0, length)
    wave_x = lane_wave((block, length), 0, col * block, length)
    kappa_y = wave_y.astype(jnp.float32) / (length // 2)
    kappa_x = wave_x.astype(jnp.float32) / (length // 2)
    damping = jnp.exp(-viscosity * time_step * (kappa_x * kappa_x + kappa_y * kappa_y))
    retained = (3 * jnp.abs(wave_x) < length) & (3 * jnp.abs(wave_y) < length)
    for f in range(3):
        real = parts[f * wide : f * wide + block]
        imag = parts[f * wide + block : (f + 1) * wide]
        forcing_real = real[:, :length] + imag[:, length:]
        forcing_imag = imag[:, :length] - real[:, length:]
        out[f, 0, 0] = damping * (
            spectra[f, 0, 0] + time_step * jnp.where(retained, forcing_real, 0.0)
        )
        out[f, 1, 0] = damping * (
            spectra[f, 1, 0] + time_step * jnp.where(retained, forcing_imag, 0.0)
        )


def whole_spec(shape):
    return pl.BlockSpec(shape, lambda *_: (0,) * len(shape))


def kernel_call(body, scalars, operands, specs, out_shapes, scratch=(), cost=None):
    out_shapes = [
        jax.ShapeDtypeStruct(s, jnp.float32) if isinstance(s, tuple) else s for s in out_shapes
    ]
    return pl.pallas_call(
        body,
        grid=(1,),
        in_specs=[pl.BlockSpec(memory_space=pltpu.SMEM)] * len(scalars) + specs,
        out_specs=[whole_spec(s.shape) for s in out_shapes],
        out_shape=out_shapes,
        scratch_shapes=list(scratch),
        compiler_params=pltpu.CompilerParams(vmem_limit_bytes=20 * 1024 * 1024),
        cost_estimate=cost,
    )(*scalars, *operands)


def needed_routes(count, needed):
    pairs = [[int(needed[d] and i != d) for d in range(count)] for i in range(count)]
    spare = [i for i in range(count) for _ in range(count - 1 - sum(pairs[i]))]
    idle = [d for d in range(count) if not needed[d] for _ in range(count - 1)]
    for i, d in zip(spare, idle):
        pairs[i][d] += 1
    far = [[2 * abs(i - d) if needed[d] else 0 for d in range(count)] for i in range(count)]
    routes = []
    for _ in range(count - 1):
        best = max(
            (
                p
                for p in itertools.permutations(range(count))
                if all(pairs[i][p[i]] for i in range(count))
            ),
            key=lambda p: sum(far[i][p[i]] for i in range(count)),
        )
        for i, d in enumerate(best):
            pairs[i][d] -= 1
        routes.append(best)
    return routes


def route_table(routes):
    count = len(routes[0])
    targets = [list(range(count))] + [list(r) for r in routes]
    sources = [[t.index(i) for i in range(count)] for t in targets]
    return jnp.asarray(np.array([targets, sources], np.int32))


def exchange(slabs, axis, routes):
    arrived = [slabs[0]]
    for slab, route in zip(slabs[1:], routes):
        arrived.append(lax.ppermute(slab, axis, list(enumerate(route))))
    return arrived


def fast_device(velocity_hat, scalar, tile_offset):
    return fast_step(velocity_hat, scalar, tile_offset)


def fast_step(velocity_hat, scalar, tile_offset):
    length = velocity_hat.shape[4]
    block = velocity_hat.shape[3]
    planes, height, breadth = scalar.shape
    count = lax.axis_size("col")
    rows = lax.axis_size("row")
    wide = 2 * block
    wave = np.arange(length)
    wave = np.where(wave < length // 2, wave, wave - length)
    kept = (3 * np.abs(wave) < length).reshape(count, block).any(axis=1)
    departure_routes = needed_routes(count, kept.tolist())
    departures = route_table(departure_routes)
    y_high, y_low = [jnp.asarray(t) for t in y_table(length)]
    half = count // 2
    far, near = list(range(half, count)), list(range(half))
    slab_shape = (5 * block + 8, wide)
    edge_shape = (planes, 8, breadth)
    hbm = pl.BlockSpec(memory_space=pltpu.HBM)

    def spectral_lines(deltas, edges):
        return kernel_call(
            functools.partial(inverse_y, count, block, length, deltas),
            [],
            [
                pltpu.with_memory_space_constraint(x, pltpu.HBM)
                for x in (velocity_hat, scalar, y_high, y_low)
            ],
            [hbm] * 4,
            [slab_shape] * len(deltas) + [edge_shape] * edges,
            [
                pltpu.VMEM(velocity_hat.shape, jnp.float32),
                pltpu.VMEM((half * block + 2 * margin, 2 * length), jnp.bfloat16),
                pltpu.VMEM((half * block + 2 * margin, 2 * length), jnp.bfloat16),
                pltpu.SemaphoreType.DMA((5,)),
                pltpu.VMEM((10 * block, 2 * length), jnp.bfloat16),
                pltpu.VMEM((10 * block, 2 * length), jnp.bfloat16),
                pltpu.VMEM((half * block + 2 * margin, 10 * block), jnp.float32),
            ],
        )

    def xor_routes(deltas):
        return [tuple(i ^ d for i in range(count)) for d in deltas]

    far_slabs = spectral_lines(far, 0)
    far_slabs = exchange([None, *far_slabs], "col", xor_routes(far))[1:]
    *near_slabs, tail, head = spectral_lines(near, 2)
    near_slabs = exchange(near_slabs, "col", xor_routes(near[1:]))
    upper, lower = exchange(
        [None, tail, head], "col", [tuple((i + s) % count for i in range(count)) for s in (1, -1)]
    )[1:]
    lhs = [pltpu.VMEM((6 * block + 16, length), jnp.bfloat16)] * 2
    near_sum, x_high, x_low = kernel_call(
        functools.partial(partial_x, count, block, length, near),
        [],
        [*near_slabs, y_high, y_low],
        [whole_spec(x.shape) for x in (*near_slabs, y_high, y_low)],
        [
            (6 * block + 16, length),
            jax.ShapeDtypeStruct((2 * length, length), jnp.bfloat16),
            jax.ShapeDtypeStruct((2 * length, length), jnp.bfloat16),
        ],
        lhs,
    )
    lines = block + 8
    columns = -(-(breadth // 2 + 3) // wide) * wide
    window_rows = 2 * lines * (columns // wide) + planes * (height + 8)
    results = kernel_call(
        functools.partial(middle, count, rows, block, length, planes, breadth, far),
        [tile_offset, departures],
        [*far_slabs, near_sum, upper, lower, scalar, scalar, x_high, x_low],
        [whole_spec(x.shape) for x in (*far_slabs, near_sum, upper, lower)]
        + [
            pl.BlockSpec((planes, height, wide), lambda *_: (0, 0, 0)),
            pl.BlockSpec((planes, height, wide), lambda *_: (0, 0, breadth // wide - 1)),
            whole_spec(x_high.shape),
            whole_spec(x_low.shape),
        ],
        [(3 * block, wide)] * count + [(window_rows, wide)] * rows + [edge_shape],
        lhs + [pltpu.VMEM((3 * block, 2 * length), jnp.float32)],
    )
    windows = exchange(results[count : count + rows], "row", [
        tuple((i + s) % rows for i in range(rows)) for s in range(1, rows)
    ])
    returned = exchange(results[:count], "col", departure_routes)
    rim = results[count + rows]
    weights = [
        jnp.asarray(row_weights(block, height, block, block + 7)),
        jnp.asarray(row_weights(block, height, block + 2, block + 6)),
    ]
    (scalar_new,) = kernel_call(
        functools.partial(transport, rows, block, planes),
        [],
        [scalar, rim, *windows, *weights],
        [whole_spec(x.shape) for x in (scalar, rim, *windows, *weights)],
        [scalar.shape],
        cost=pl.CostEstimate(flops=4_000_000_000, bytes_accessed=0, transcendentals=0),
    )
    (velocity_new,) = kernel_call(
        functools.partial(forward_y, count, block, length),
        [departures],
        [*returned, velocity_hat, y_high, y_low],
        [whole_spec(x.shape) for x in (*returned, velocity_hat, y_high, y_low)],
        [velocity_hat.shape],
        [pltpu.VMEM((length, 3 * wide), jnp.float32)],
    )
    return velocity_new, scalar_new


def fits(mesh, velocity_hat, scalar):
    count, rows = mesh.shape["col"], mesh.shape["row"]
    planes = velocity_hat.shape[2] // (mesh.shape["group"] * rows)
    length = velocity_hat.shape[4]
    block = velocity_hat.shape[3] // count
    height, breadth = scalar.shape[1] // count, scalar.shape[2] // rows
    return (
        planes == 1
        and count in (4, 8)
        and 1 < rows <= 8
        and (2 * block) % 128 == 0
        and height == 2 * block
        and breadth * rows == 2 * length
        and breadth % (2 * block) == 0
        and breadth // 2 + 3 <= length
    )


def solution(mesh):
    def step(velocity_hat, scalar, tile_offset):
        fast = fits(mesh, velocity_hat, scalar)
        mapped = jax.shard_map(
            fast_device if fast else per_device,
            mesh=mesh,
            in_specs=(P(None, None, ("group", "row"), "col", None), P("group", "col", "row"), P()),
            out_specs=(P(None, None, ("group", "row"), "col", None), P("group", "col", "row")),
            check_vma=False,
        )
        return mapped(velocity_hat, scalar, tile_offset)

    return step
```

```python
import functools
import math

import jax
import jax.numpy as jnp
import numpy as np
from jax import lax
from jax.experimental import pallas as pl
from jax.experimental.pallas import tpu as pltpu
from jax.sharding import PartitionSpec as P


time_step = 0.25
viscosity = 2.0
diffusivity = 0.15
substep = 0.2
highest = lax.Precision.HIGHEST


def extended(cells, sides, width):
    for axis, dim in sides:
        count = lax.axis_size(axis)
        head = lax.slice_in_dim(cells, 0, width, axis=dim)
        tail = lax.slice_in_dim(cells, cells.shape[dim] - width, cells.shape[dim], axis=dim)
        cells = jnp.concatenate(
            [
                lax.ppermute(tail, axis, [(i, (i + 1) % count) for i in range(count)]),
                cells,
                lax.ppermute(head, axis, [((i + 1) % count, i) for i in range(count)]),
            ],
            axis=dim,
        )
    return cells


def dft_tables(length):
    indices = jnp.arange(length, dtype=jnp.int32)
    phases = indices[:, None] * indices[None, :] % length
    angles = phases.astype(jnp.float32) * (2.0 * math.pi / length)
    factor = 1.0 / math.sqrt(length)
    return (jnp.cos(angles) * factor, jnp.sin(angles) * factor)


def signed_wave(indices, length):
    return jnp.where(indices < length // 2, indices, indices - length)


def transpose_col(packed):
    return lax.all_to_all(packed, "col", split_axis=3, concat_axis=4, tiled=True)


def refine_rows(coarse, margin):
    current = coarse[:, :-1, :]
    following = coarse[:, 1:, :]
    paired = jnp.stack([current, (current + following) * 0.5], axis=2)
    refined = paired.reshape(coarse.shape[0], 2 * (coarse.shape[1] - 1), coarse.shape[2])
    height = 2 * (coarse.shape[1] - 2 * margin)
    return refined[:, margin : margin + height + 2 * margin, :]


def advance(values, x_speed, y_speed):
    height = values.shape[1] - 4
    breadth = values.shape[2] - 4

    def neighbor(step_y, step_x):
        return values[:, 2 + step_y : 2 + step_y + height, 2 + step_x : 2 + step_x + breadth]

    center = neighbor(0, 0)
    grad_x = (neighbor(0, -2) - neighbor(0, 2) + 8.0 * (neighbor(0, 1) - neighbor(0, -1))) / 12.0
    grad_y = (neighbor(-2, 0) - neighbor(2, 0) + 8.0 * (neighbor(1, 0) - neighbor(-1, 0))) / 12.0
    lap_x = (
        16.0 * (neighbor(0, 1) + neighbor(0, -1)) - neighbor(0, 2) - neighbor(0, -2) - 30.0 * center
    ) / 12.0
    lap_y = (
        16.0 * (neighbor(1, 0) + neighbor(-1, 0)) - neighbor(2, 0) - neighbor(-2, 0) - 30.0 * center
    ) / 12.0
    return center + substep * (
        diffusivity * (lap_x + lap_y) - (x_speed * grad_x + y_speed * grad_y)
    )


def per_device(velocity_hat, scalar, tile_offset):
    extent = velocity_hat.shape[4]
    kx_block = velocity_hat.shape[3]
    cosine_table, sine_table = dft_tables(extent)
    wave_all = signed_wave(jnp.arange(extent, dtype=jnp.int32), extent)
    local_wave = signed_wave(
        lax.axis_index("col") * kx_block + jnp.arange(kx_block, dtype=jnp.int32), extent
    )
    kappa_y = (wave_all.astype(jnp.float32) / (extent // 2))[None, None, :]
    kappa_x = (local_wave.astype(jnp.float32) / (extent // 2))[None, :, None]
    real_part = velocity_hat[:, 0]
    imag_part = velocity_hat[:, 1]
    spin_x_real = -kappa_y * imag_part[2]
    spin_x_imag = kappa_y * real_part[2]
    spin_z_real = kappa_y * imag_part[0] - kappa_x * imag_part[1]
    spin_z_imag = kappa_x * real_part[1] - kappa_y * real_part[0]
    fields_real = jnp.concatenate([real_part, jnp.stack([spin_x_real, spin_z_real])])
    fields_imag = jnp.concatenate([imag_part, jnp.stack([spin_x_imag, spin_z_imag])])
    lines_real = jnp.einsum(
        "fpkq,qy->fpyk", fields_real, cosine_table, precision=highest
    ) - jnp.einsum("fpkq,qy->fpyk", fields_imag, sine_table, precision=highest)
    lines_imag = jnp.einsum(
        "fpkq,qy->fpyk", fields_real, sine_table, precision=highest
    ) + jnp.einsum("fpkq,qy->fpyk", fields_imag, cosine_table, precision=highest)
    landed = transpose_col(jnp.stack([lines_real, lines_imag], axis=1))
    landed_real = landed[:, 0]
    landed_imag = landed[:, 1]
    wave_x = (wave_all.astype(jnp.float32) / (extent // 2))[None, None, :]
    spin_y_real = wave_x * landed_imag[2]
    spin_y_imag = -wave_x * landed_real[2]
    landed_real = jnp.concatenate([landed_real[:4], spin_y_real[None], landed_real[4:]])
    landed_imag = jnp.concatenate([landed_imag[:4], spin_y_imag[None], landed_imag[4:]])
    physical = jnp.einsum(
        "fpyk,kx->fpyx", landed_real, cosine_table, precision=highest
    ) - jnp.einsum("fpyk,kx->fpyx", landed_imag, sine_table, precision=highest)
    x_speed = physical[0]
    y_speed = physical[1]
    z_speed = physical[2]
    omega_x = physical[3]
    omega_y = physical[4]
    omega_z = physical[5]
    product = jnp.stack(
        [
            y_speed * omega_z - z_speed * omega_y,
            z_speed * omega_x - x_speed * omega_z,
            x_speed * omega_y - y_speed * omega_x,
        ]
    )
    rows_real = jnp.einsum("cpyx,xk->cpky", product, cosine_table, precision=highest)
    rows_imag = -jnp.einsum("cpyx,xk->cpky", product, sine_table, precision=highest)
    returned = transpose_col(jnp.stack([rows_real, rows_imag], axis=1))
    back_real = returned[:, 0]
    back_imag = returned[:, 1]
    forcing_real = jnp.einsum(
        "cpky,yq->cpkq", back_real, cosine_table, precision=highest
    ) + jnp.einsum("cpky,yq->cpkq", back_imag, sine_table, precision=highest)
    forcing_imag = jnp.einsum(
        "cpky,yq->cpkq", back_imag, cosine_table, precision=highest
    ) - jnp.einsum("cpky,yq->cpkq", back_real, sine_table, precision=highest)
    retained = (3 * jnp.abs(local_wave)[:, None] < extent) & (
        3 * jnp.abs(wave_all)[None, :] < extent
    )
    damping = jnp.exp(-viscosity * time_step * (kappa_x**2 + kappa_y**2))
    new_real = damping * (real_part + time_step * jnp.where(retained, forcing_real, 0.0))
    new_imag = damping * (imag_part + time_step * jnp.where(retained, forcing_imag, 0.0))
    velocity_new = jnp.stack([new_real, new_imag], axis=1)
    horizontal = physical[:2]
    doubled = jnp.concatenate([horizontal, horizontal], axis=3)
    shifted = lax.dynamic_slice_in_dim(doubled, tile_offset[0], extent, 3)
    following = jnp.concatenate([shifted[..., 1:], shifted[..., :1]], axis=3)
    refined_x = jnp.stack([shifted, (shifted + following) * 0.5], axis=4).reshape(
        2, shifted.shape[1], shifted.shape[2], 2 * extent
    )
    arrived = lax.all_to_all(refined_x, "row", split_axis=3, concat_axis=1, tiled=True)
    scalar_ext, x_coarse, y_coarse = (
        extended(scalar, (("row", 2), ("col", 1)), 2),
        extended(arrived[0], (("row", 2), ("col", 1)), 2),
        extended(arrived[1], (("row", 2), ("col", 1)), 2),
    )
    x_refined = refine_rows(x_coarse, 2)[:, 2:-2, 2:-2]
    y_refined = refine_rows(y_coarse, 2)[:, 2:-2, 2:-2]
    halfway = advance(scalar_ext, x_refined, y_refined)
    halfway_ext = extended(halfway, (("row", 2), ("col", 1)), 2)
    scalar_new = advance(halfway_ext, x_refined, y_refined)
    return (velocity_new, scalar_new)


def split(values):
    high = values.astype(jnp.bfloat16)
    return high, (values - high.astype(jnp.float32)).astype(jnp.bfloat16)


def host_split(table):
    table = table.astype(np.float32)
    high = table.astype(jnp.bfloat16)
    return high, (table - high.astype(np.float32)).astype(jnp.bfloat16)


def host_angles(rows, columns, length):
    phases = np.outer(rows, columns) % length
    return phases * (2.0 * np.pi / length)


margin = 16


def y_table(length):
    rows = np.arange(-margin, length + margin) % length
    angles = host_angles(rows, np.arange(length), length)
    return host_split(np.concatenate([np.cos(angles), np.sin(angles)], axis=1) / np.sqrt(length))


def row_weights(lines, height, next_at, last_at):
    weights = np.zeros((height + 8, lines + 8), np.float32)
    place = {**{j: j for j in range(lines)}, lines: next_at, lines + 1: next_at + 1, -1: last_at}
    for fine in range(-2, height + 2):
        base = fine // 2
        row = fine if fine >= 0 else height + 8 + fine
        if fine % 2 == 0:
            weights[row, place[base]] += 1.0
        else:
            weights[row, place[base]] += 0.5
            weights[row, place[base + 1]] += 0.5
    return weights.astype(jnp.bfloat16)


def column_weights(columns, breadth, total):
    base = lax.broadcasted_iota(jnp.int32, (columns, total), 0) - 1
    fine = lax.broadcasted_iota(jnp.int32, (columns, total), 1)
    fine = jnp.where(fine < breadth + 2, fine, fine - total)
    twice = jnp.abs(2 * base - fine)
    at_point = jnp.where(fine % 2 == 0, jnp.where(twice == 0, 1.0, 0.0), jnp.where(twice == 1, 0.5, 0.0))
    return jnp.where(fine >= -2, at_point, 0.0).astype(jnp.bfloat16)


def dot(left, right, contract):
    return lax.dot_general(
        left, right, (contract, ((), ())), preferred_element_type=jnp.float32
    )


def dot3(left, right, contract):
    return (
        dot(left[0], right[0], contract)
        + dot(left[0], right[1], contract)
        + dot(left[1], right[0], contract)
    )


def lane_wave(shape, dim, start, length):
    wave = lax.broadcasted_iota(jnp.int32, shape, dim) + start
    return jnp.where(wave < length // 2, wave, wave - length)


def inverse_y(count, block, length, deltas, spectra_in, scalar_in, high_in, low_in, *rest):
    outs, edges = rest[: len(deltas)], rest[len(deltas) : -7]
    spectra, table_high, table_low, sems, spectra_high, spectra_low, lines = rest[-7:]
    height = scalar_in.shape[1]
    col = lax.axis_index("col")
    half = count // 2
    reach = half * block
    side = lax.div(lax.bitwise_xor(col, deltas[0]), half)
    rows = pl.ds(pl.multiple_of(side * reach, 16), reach + 2 * margin)
    pieces = [
        (spectra_in, spectra),
        (high_in.at[rows, :], table_high),
        (low_in.at[rows, :], table_low),
    ]
    if edges:
        pieces += [
            (scalar_in.at[:, height - 8 : height, :], edges[0]),
            (scalar_in.at[:, 0:8, :], edges[1]),
        ]
    copies = [
        pltpu.make_async_copy(source, target, sems.at[n])
        for n, (source, target) in enumerate(pieces)
    ]
    for copy in copies:
        copy.start()
    kappa_y = lane_wave((block, length), 1, 0, length).astype(jnp.float32) / (length // 2)
    kappa_x = lane_wave((block, length), 0, col * block, length).astype(jnp.float32) / (length // 2)
    copies[0].wait()
    real = [spectra[f, 0, 0] for f in range(3)]
    imag = [spectra[f, 1, 0] for f in range(3)]
    real.append(-kappa_y * imag[2])
    imag.append(kappa_y * real[2])
    real.append(kappa_y * imag[0] - kappa_x * imag[1])
    imag.append(kappa_x * real[1] - kappa_y * real[0])
    for f in range(5):
        real_pair = split(real[f])
        imag_pair = split(imag[f])
        top = slice(2 * f * block, (2 * f + 1) * block)
        bottom = slice((2 * f + 1) * block, (2 * f + 2) * block)
        for store, re, im in (
            (spectra_high, real_pair[0], imag_pair[0]),
            (spectra_low, real_pair[1], imag_pair[1]),
        ):
            store[top, :length] = re
            store[top, length:] = -im
            store[bottom, :length] = im
            store[bottom, length:] = re
    for copy in copies[1:]:
        copy.wait()
    lines[...] = dot3(
        (table_high[...], table_low[...]), (spectra_high[...], spectra_low[...]), ((1,), (1,))
    )
    wide = 2 * block
    sub = lax.broadcasted_iota(jnp.int32, (8, wide), 0)
    for delta, out in zip(deltas, outs):
        dest = lax.bitwise_and(lax.bitwise_xor(col, delta), half - 1)
        base = pl.multiple_of(margin + dest * block, 8)
        for f in range(5):
            out[f * block : (f + 1) * block, :] = lines[
                pl.ds(base, block), f * wide : (f + 1) * wide
            ]
        following, before = pl.ds(base + block, 8), pl.ds(base - 8, 8)
        next_x = lines[following, 0:wide]
        next_y = pltpu.roll(lines[following, wide : 2 * wide], 2, 0)
        last_x = lines[before, 0:wide]
        last_y = pltpu.roll(lines[before, wide : 2 * wide], 7, 0)
        rim = jnp.where(sub < 2, next_x, jnp.where(sub < 4, next_y, jnp.where(sub < 7, last_y, last_x)))
        out[5 * block : 5 * block + 8, :] = rim


def place_slabs(count, block, length, deltas, slabs, lhs_high, lhs_low):
    col = lax.axis_index("col")
    wide = 2 * block
    lane = lax.broadcasted_iota(jnp.int32, (1, wide), 1)
    for delta, slab in zip(deltas, slabs):
        source = lax.bitwise_xor(col, delta)
        at = pl.ds(pl.multiple_of(lax.bitwise_and(source, count // 2 - 1) * wide, wide), wide)
        value = slab[0 : 5 * block, :]
        high, low = split(value)
        lhs_high[0 : 5 * block, at] = high
        lhs_low[0 : 5 * block, at] = low
        wave = lax.rem(lane, block) + source * block
        wave = jnp.where(wave < length // 2, wave, wave - length)
        kappa = wave.astype(jnp.float32) / (length // 2)
        kappa = jnp.where(lane < block, kappa, -kappa)
        spin = jnp.concatenate(
            [
                pltpu.roll(value[2 * block : 3 * block], block, 1) * kappa,
                slab[5 * block : 5 * block + 8, :],
                jnp.zeros((8, wide), jnp.float32),
            ]
        )
        high, low = split(spin)
        lhs_high[5 * block :, at] = high
        lhs_low[5 * block :, at] = low


def partial_x(count, block, length, deltas, *refs):
    slabs = refs[: len(deltas)]
    y_high, y_low, out, table_high, table_low, lhs_high, lhs_low = refs[len(deltas) :]
    col = lax.axis_index("col")
    for source, target in ((y_high, table_high), (y_low, table_low)):
        for c in range(count):
            rows = slice(margin + c * block, margin + (c + 1) * block)
            target[2 * c * block : (2 * c + 1) * block, :] = source[rows, 0:length]
            target[(2 * c + 1) * block : (2 * c + 2) * block, :] = -source[rows, length:]
    place_slabs(count, block, length, deltas, slabs, lhs_high, lhs_low)
    side = lax.div(lax.bitwise_xor(col, deltas[0]), count // 2)
    rows = pl.ds(pl.multiple_of(side * length, 16), length)
    out[...] = dot3(
        (lhs_high[...], lhs_low[...]), (table_high[rows, :], table_low[rows, :]), ((1,), (0,))
    )


def middle(count, rows, block, length, breadth, deltas, offsets, departures, *refs):
    slabs = refs[: len(deltas)]
    near_sum, table_high, table_low = refs[len(deltas) : len(deltas) + 3]
    refs = refs[len(deltas) + 3 :]
    outs, windows = refs[:count], refs[count : count + rows]
    lhs_high, lhs_low, freq = refs[count + rows :]
    col, row, offset = lax.axis_index("col"), lax.axis_index("row"), offsets[0]
    wide = 2 * block
    lane = lax.broadcasted_iota(jnp.int32, (1, wide), 1)
    place_slabs(count, block, length, deltas, slabs, lhs_high, lhs_low)
    side = lax.div(lax.bitwise_xor(col, deltas[0]), count // 2)
    half_rows = pl.ds(pl.multiple_of(side * length, 16), length)
    physical = near_sum[...] + dot3(
        (lhs_high[...], lhs_low[...]),
        (table_high[half_rows, :], table_low[half_rows, :]),
        ((1,), (0,)),
    )
    table = (table_high[...], table_low[...])
    u, v, w, spin_x, spin_z, spin_y = [physical[f * block : (f + 1) * block] for f in range(6)]
    product = jnp.concatenate([v * spin_z - w * spin_y, w * spin_x - u * spin_z, u * spin_y - v * spin_x])
    freq[...] = dot3(split(product), table, ((1,), (1,)))
    for s in range(count):
        at = pl.multiple_of(departures[0, s, col] * wide, wide)
        outs[s][...] = freq[:, pl.ds(at, wide)]
    rim = physical[6 * block : 6 * block + 8]
    cells = breadth // 2
    lines = block + 8
    span = windows[0].shape[0] // (2 * lines)
    for s in range(rows):
        target = lax.rem(row + s, rows)
        shift = lax.rem(2 * length + 1 - offset - target * cells, length)
        for f, field in enumerate((u, v)):
            rolled = pltpu.roll(jnp.concatenate([field, rim]), shift, 1)
            for b in range(span):
                at = (f * span + b) * lines
                windows[s][at : at + lines, :] = rolled[:, b * wide : (b + 1) * wide]


def pack_edges(block, planes, upper, lower, first, final, rim_out, packed, across):
    wide = 2 * block
    height, breadth = first.shape[1], rim_out.shape[2]
    lane = lax.broadcasted_iota(jnp.int32, (1, wide), 1)
    sub = lax.broadcasted_iota(jnp.int32, (8, breadth), 0)
    across[...] = column_weights(across.shape[0], breadth, breadth + wide)
    for p in range(planes):
        rim = jnp.where(sub < 4, lower[p], upper[p])
        rim_out[p] = rim
        at = p * (height + 8)
        packed[at : at + height, :] = jnp.where(lane < block, first[p], final[p])
        packed[at + height : at + height + 8, :] = jnp.where(
            lane < block, rim[:, 0:wide], rim[:, breadth - wide :]
        )


def transport(rows, block, parts, scalar, rim, from_left, from_right, *refs):
    windows = refs[: len(parts)]
    weights_x, weights_y, across = refs[len(parts) : len(parts) + 3]
    out, stage, sems = refs[-3:]
    row = lax.axis_index("row")
    wide = 2 * block
    height, breadth = scalar.shape[1], scalar.shape[2]
    lines = block + 8
    span = windows[0].shape[0] // (2 * lines)
    lane = lax.broadcasted_iota(jnp.int32, (1, wide), 1)
    tall = height + 8

    def shifted(values, amount, axis):
        return pltpu.roll(values, (-amount) % values.shape[axis], axis)

    copies = []
    for n, s in enumerate(parts):
        p = lax.rem(row + rows - s, rows)
        speeds = []
        for f, weights in enumerate((weights_x, weights_y)):
            coarse = jnp.concatenate(
                [
                    windows[n][(f * span + b) * lines : (f * span + b + 1) * lines, :]
                    for b in range(span)
                ],
                axis=1,
            )
            high, low = split(coarse)
            taller = dot(weights[...], high, ((1,), (0,))) + dot(weights[...], low, ((1,), (0,)))
            high, low = split(taller)
            speeds.append(
                dot(high, across[...], ((1,), (0,))) + dot(low, across[...], ((1,), (0,)))
            )
        x_speed, y_speed = speeds
        at = pl.ds(pl.multiple_of(p * tall, 8), tall)
        values = jnp.concatenate(
            [
                jnp.concatenate([scalar[p], rim[p]], axis=0),
                jnp.where(lane < block, from_right[at, :], from_left[at, :]),
            ],
            axis=1,
        )
        for _ in range(2):
            right, left = shifted(values, 1, 1), shifted(values, -1, 1)
            right2, left2 = shifted(values, 2, 1), shifted(values, -2, 1)
            below, above = shifted(values, 1, 0), shifted(values, -1, 0)
            below2, above2 = shifted(values, 2, 0), shifted(values, -2, 0)
            grad_x = left2 - right2 + 8.0 * (right - left)
            grad_y = above2 - below2 + 8.0 * (below - above)
            near = (right + left) + (below + above)
            far = (right2 + left2) + (below2 + above2)
            spread = 16.0 * near - far - 60.0 * values
            values = values + (substep / 12.0) * (
                diffusivity * spread - (x_speed * grad_x + y_speed * grad_y)
            )
        stage[n] = values[:height, :breadth]
        copies.append(pltpu.make_async_copy(stage.at[n], out.at[p], sems.at[n]))
        copies[-1].start()
    for copy in copies:
        copy.wait()


def forward_y(count, block, length, departures, *refs):
    slabs = refs[:count]
    spectra, table_high, table_low, out, gathered, stage, sems = refs[count:]
    col = lax.axis_index("col")
    wide = 2 * block
    for s in range(count):
        at = pl.multiple_of(departures[1, s, col] * block, 8)
        for f in range(3):
            gathered[pl.ds(at, block), f * wide : (f + 1) * wide] = slabs[s][
                f * block : (f + 1) * block, :
            ]
    inner = slice(margin, margin + length)
    table = (table_high[inner, :], table_low[inner, :])
    wave_y = lane_wave((block, length), 1, 0, length)
    wave_x = lane_wave((block, length), 0, col * block, length)
    kappa_y = wave_y.astype(jnp.float32) / (length // 2)
    kappa_x = wave_x.astype(jnp.float32) / (length // 2)
    damping = jnp.exp(-viscosity * time_step * (kappa_x * kappa_x + kappa_y * kappa_y))
    retained = (3 * jnp.abs(wave_x) < length) & (3 * jnp.abs(wave_y) < length)
    copies = []
    for f in range(3):
        parts = dot3(split(gathered[:, f * wide : (f + 1) * wide].T), table, ((1,), (0,)))
        real, imag = parts[:block], parts[block:]
        forcing_real = real[:, :length] + imag[:, length:]
        forcing_imag = imag[:, :length] - real[:, length:]
        stage[f, 0, 0] = damping * (
            spectra[f, 0, 0] + time_step * jnp.where(retained, forcing_real, 0.0)
        )
        stage[f, 1, 0] = damping * (
            spectra[f, 1, 0] + time_step * jnp.where(retained, forcing_imag, 0.0)
        )
        copies.append(pltpu.make_async_copy(stage.at[f], out.at[f], sems.at[f]))
        copies[-1].start()
    for copy in copies:
        copy.wait()


def whole_spec(shape):
    return pl.BlockSpec(shape, lambda *_: (0,) * len(shape))


def kernel_call(body, scalars, operands, specs, out_shapes, scratch=(), cost=None):
    out_shapes = [
        jax.ShapeDtypeStruct(s, jnp.float32) if isinstance(s, tuple) else s for s in out_shapes
    ]
    return pl.pallas_call(
        body,
        grid=(1,),
        in_specs=[pl.BlockSpec(memory_space=pltpu.SMEM)] * len(scalars) + specs,
        out_specs=[whole_spec(s.shape) for s in out_shapes],
        out_shape=out_shapes,
        scratch_shapes=list(scratch),
        compiler_params=pltpu.CompilerParams(vmem_limit_bytes=20 * 1024 * 1024),
        cost_estimate=cost,
    )(*scalars, *operands)


def needed_routes(count, needed):
    half = count // 2
    routes = []
    for delta in [*range(half, count), *range(1, half)]:
        route = [i ^ delta for i in range(count)]
        low = [i for i in range(half) if route[i] >= half and not needed[route[i]]]
        high = [i for i in range(half, count) if route[i] < half and not needed[route[i]]]
        for i, j in zip(low, high):
            route[i], route[j] = route[j], route[i]
        routes.append(tuple(route))
    return routes


def route_table(routes):
    count = len(routes[0])
    targets = [list(range(count))] + [list(r) for r in routes]
    sources = [[t.index(i) for i in range(count)] for t in targets]
    return jnp.asarray(np.array([targets, sources], np.int32))


def exchange(slabs, axis, routes):
    arrived = [slabs[0]]
    for slab, route in zip(slabs[1:], routes):
        arrived.append(lax.ppermute(slab, axis, list(enumerate(route))))
    return arrived


def fast_device(velocity_hat, scalar, tile_offset):
    return fast_step(velocity_hat, scalar, tile_offset)


def fast_step(velocity_hat, scalar, tile_offset):
    length = velocity_hat.shape[4]
    block = velocity_hat.shape[3]
    planes, height, breadth = scalar.shape
    count = lax.axis_size("col")
    rows = lax.axis_size("row")
    wide = 2 * block
    wave = np.arange(length)
    wave = np.where(wave < length // 2, wave, wave - length)
    kept = (3 * np.abs(wave) < length).reshape(count, block).any(axis=1)
    departure_routes = needed_routes(count, kept.tolist())
    departures = route_table(departure_routes)
    y_high, y_low = [jnp.asarray(t) for t in y_table(length)]
    half = count // 2
    far, near = list(range(half, count)), list(range(half))
    slab_shape = (5 * block + 8, wide)
    edge_shape = (planes, 8, breadth)
    hbm = pl.BlockSpec(memory_space=pltpu.HBM)

    def spectral_lines(deltas, edges):
        return kernel_call(
            functools.partial(inverse_y, count, block, length, deltas),
            [],
            [
                pltpu.with_memory_space_constraint(x, pltpu.HBM)
                for x in (velocity_hat, scalar, y_high, y_low)
            ],
            [hbm] * 4,
            [slab_shape] * len(deltas) + [edge_shape] * edges,
            [
                pltpu.VMEM(velocity_hat.shape, jnp.float32),
                pltpu.VMEM((half * block + 2 * margin, 2 * length), jnp.bfloat16),
                pltpu.VMEM((half * block + 2 * margin, 2 * length), jnp.bfloat16),
                pltpu.SemaphoreType.DMA((5,)),
                pltpu.VMEM((10 * block, 2 * length), jnp.bfloat16),
                pltpu.VMEM((10 * block, 2 * length), jnp.bfloat16),
                pltpu.VMEM((half * block + 2 * margin, 10 * block), jnp.float32),
            ],
        )

    def xor_routes(deltas):
        return [tuple(i ^ d for i in range(count)) for d in deltas]

    far_slabs = spectral_lines(far, 0)
    far_slabs = exchange([None, *far_slabs], "col", xor_routes(far))[1:]
    *near_slabs, tail, head = spectral_lines(near, 2)
    near_slabs = exchange(near_slabs, "col", xor_routes(near[1:]))
    upper, lower = exchange(
        [None, tail, head], "col", [tuple((i + s) % count for i in range(count)) for s in (1, -1)]
    )[1:]
    lhs = [pltpu.VMEM((6 * block + 16, length), jnp.bfloat16)] * 2
    near_sum, x_high, x_low = kernel_call(
        functools.partial(partial_x, count, block, length, near),
        [],
        [*near_slabs, y_high, y_low],
        [whole_spec(x.shape) for x in (*near_slabs, y_high, y_low)],
        [
            (6 * block + 16, length),
            jax.ShapeDtypeStruct((2 * length, length), jnp.bfloat16),
            jax.ShapeDtypeStruct((2 * length, length), jnp.bfloat16),
        ],
        lhs,
    )
    lines = block + 8
    columns = -(-(breadth // 2 + 3) // wide) * wide
    window_rows = 2 * lines * (columns // wide)
    row_routes = [tuple((i + s) % rows for i in range(rows)) for s in range(1, rows)]
    rim, packed, across = kernel_call(
        functools.partial(pack_edges, block, planes),
        [],
        [upper, lower, scalar, scalar],
        [
            whole_spec(upper.shape),
            whole_spec(lower.shape),
            pl.BlockSpec((planes, height, wide), lambda *_: (0, 0, 0)),
            pl.BlockSpec((planes, height, wide), lambda *_: (0, 0, breadth // wide - 1)),
        ],
        [
            edge_shape,
            (planes * (height + 8), wide),
            jax.ShapeDtypeStruct((columns, breadth + wide), jnp.bfloat16),
        ],
    )
    sides = exchange([packed] * rows, "row", row_routes)
    results = kernel_call(
        functools.partial(middle, count, rows, block, length, breadth, far),
        [tile_offset, departures],
        [*far_slabs, near_sum, x_high, x_low],
        [whole_spec(x.shape) for x in (*far_slabs, near_sum, x_high, x_low)],
        [(3 * block, wide)] * count + [(window_rows, wide)] * rows,
        lhs + [pltpu.VMEM((3 * block, 2 * length), jnp.float32)],
    )
    windows = exchange(results[count : count + rows], "row", row_routes)
    returned = exchange(results[:count], "col", departure_routes)
    weights = [
        jnp.asarray(row_weights(block, height, block, block + 7)),
        jnp.asarray(row_weights(block, height, block + 2, block + 6)),
    ]
    operands = [scalar, rim, sides[1 % rows], sides[rows - 1], *windows, *weights, across]
    scalar_new = pl.pallas_call(
        functools.partial(transport, rows, block, tuple(range(rows))),
        name="transport",
        grid=(1,),
        in_specs=[whole_spec(x.shape) for x in operands],
        out_specs=hbm,
        out_shape=jax.ShapeDtypeStruct(scalar.shape, jnp.float32),
        scratch_shapes=[
            pltpu.VMEM((rows, height, breadth), jnp.float32),
            pltpu.SemaphoreType.DMA((rows,)),
        ],
        compiler_params=pltpu.CompilerParams(vmem_limit_bytes=20 * 1024 * 1024),
        cost_estimate=pl.CostEstimate(flops=4_000_000_000, bytes_accessed=0, transcendentals=0),
    )(*operands)
    operands = [*returned, velocity_hat, y_high, y_low]
    velocity_new = pl.pallas_call(
        functools.partial(forward_y, count, block, length),
        name="forward_y",
        grid=(1,),
        in_specs=[pl.BlockSpec(memory_space=pltpu.SMEM)] + [whole_spec(x.shape) for x in operands],
        out_specs=hbm,
        out_shape=jax.ShapeDtypeStruct(velocity_hat.shape, jnp.float32),
        scratch_shapes=[
            pltpu.VMEM((length, 3 * wide), jnp.float32),
            pltpu.VMEM(velocity_hat.shape, jnp.float32),
            pltpu.SemaphoreType.DMA((3,)),
        ],
        compiler_params=pltpu.CompilerParams(vmem_limit_bytes=20 * 1024 * 1024),
    )(departures, *operands)
    return velocity_new, scalar_new


def fits(mesh, velocity_hat, scalar):
    count, rows = mesh.shape["col"], mesh.shape["row"]
    planes = velocity_hat.shape[2] // (mesh.shape["group"] * rows)
    length = velocity_hat.shape[4]
    block = velocity_hat.shape[3] // count
    height, breadth = scalar.shape[1] // count, scalar.shape[2] // rows
    return (
        planes == 1
        and count in (4, 8)
        and 1 < rows <= 8
        and (2 * block) % 128 == 0
        and height == 2 * block
        and breadth * rows == 2 * length
        and breadth % (2 * block) == 0
        and breadth // 2 + 3 <= length
    )


def solution(mesh):
    def step(velocity_hat, scalar, tile_offset):
        fast = fits(mesh, velocity_hat, scalar)
        mapped = jax.shard_map(
            fast_device if fast else per_device,
            mesh=mesh,
            in_specs=(P(None, None, ("group", "row"), "col", None), P("group", "col", "row"), P()),
            out_specs=(P(None, None, ("group", "row"), "col", None), P("group", "col", "row")),
            check_vma=False,
        )
        return mapped(velocity_hat, scalar, tile_offset)

    return step
```
